32 devices in a mesh: gx: 8 (over y, x, core), gy: 4 (over z).
Axes of the slice: x: 2, y: 2, z: 4, core: 2. Of those that a mesh axis runs over, the one named last changes fastest.
Arguments:
- image: bfloat16 [32, 32, 16, 1024], P(None, 'gx', None, 'gy'), may hold values from -6 to 6
- w_first: bfloat16 [32, 32, 3, 3, 3], replicated, may hold values from -0.21875 to 0.21875
- b_first: float32 [32], replicated, may hold values from -3 to 3
- w_second: bfloat16 [64, 32, 3, 3, 3], replicated, may hold values from -0.21875 to 0.21875
- b_second: float32 [64], replicated, may hold values from -3 to 3
- w_third: bfloat16 [64, 64, 3, 3, 3], replicated, may hold values from -0.15625 to 0.15625
- b_third: float32 [64], replicated, may hold values from -3 to 3
Outputs:
- coarse_out: bfloat16 [64, 16, 8, 512], P(None, 'gx', None, 'gy')
The draws below stay inside these ranges and needn't reach their ends.
All inputs are finite; a program needn't handle non-finite values.
Results may differ from the reference program's by a relative error of at most 0.0056.
Values may be sent and summed in bfloat16 or wider, within the bound.
No kernel may reach another device: no remote copies, remote signals or barrier semaphores. Data moves between devices by JAX's collectives and lax.ppermute only.
A program may use at most 64 MiB of HBM per device.

```python
import jax
import jax.numpy as jnp
from jax import lax

C1 = 32
C2 = 64
DEPTH = 16
NXH = 32
NYH = 1024


def levels(own_key, extent, split, least, high):
    gain = 1.0
    for dim, blocks in split:
        draws = jax.random.uniform(jax.random.fold_in(jax.random.fold_in(own_key, 6), dim), (blocks,), jnp.float32, least / len(split), high / len(split))
        gain = gain * jnp.repeat(jnp.exp(draws), extent[dim] // blocks).reshape((-1,) + (1,) * (len(extent) - 1 - dim))
    return gain


def noise(rng, dims, spread, most, cuts=(), dtype=jnp.bfloat16):
    level = levels(rng, dims, cuts, -0.22, 0.18) if cuts else 1.0
    values = jax.random.normal(rng, dims, jnp.float32) * spread * level
    return jnp.minimum(jnp.maximum(values, -most), most).astype(dtype)


def setup_inputs(seed: int = 0) -> dict:
    seeds = jax.random.split(jax.random.key(seed), 8)
    return {
        "image": noise(seeds[0], (C1, NXH, DEPTH, NYH), 1.0, 6.0, ((1, 8), (3, 4))),
        "w_first": noise(seeds[1], (C1, C1, 3, 3, 3), (27 * C1) ** -0.5, 0.21875),
        "b_first": noise(seeds[2], (C1,), 0.5, 3.0, (), jnp.float32),
        "w_second": noise(seeds[3], (C2, C1, 3, 3, 3), (27 * C1) ** -0.5, 0.21875),
        "b_second": noise(seeds[4], (C2,), 0.5, 3.0, (), jnp.float32),
        "w_third": noise(seeds[5], (C2, C2, 3, 3, 3), (27 * C2) ** -0.5, 0.15625),
        "b_third": noise(seeds[6], (C2,), 0.5, 3.0, (), jnp.float32),
    }


def convolve(values, kernel, offset):
    summed = lax.conv_general_dilated(values[None], kernel, (1, 1, 1), "SAME", dimension_numbers=("NCDHW", "OIDHW", "NCDHW"), preferred_element_type=jnp.float32)[0]
    return jnp.maximum(summed + offset[:, None, None, None], 0.0)


def max_pool(values):
    chans, inline, depth, cross = values.shape
    blocks = values.reshape(chans, inline // 2, 2, depth // 2, 2, cross // 2, 2)
    return jnp.max(blocks, axis=(2, 4, 6))


def reference(image, w_first, b_first, w_second, b_second, w_third, b_third):
    layer_one = convolve(image, w_first, b_first).astype(jnp.bfloat16)
    pooled = max_pool(layer_one)
    second = convolve(pooled, w_second, b_second).astype(jnp.bfloat16)
    return convolve(second, w_third, b_third).astype(jnp.bfloat16)
```

```python
import functools

import jax
import jax.numpy as jnp
from jax import lax
from jax.experimental import pallas as pl
from jax.experimental.pallas import tpu as pltpu
from jax.sharding import PartitionSpec as P

BF = jnp.bfloat16
F32 = jnp.float32
VM = pl.BlockSpec(memory_space=pltpu.VMEM)
G = 8


def call(body, outs, scratch=(), flops=0, name=None):
    return pl.pallas_call(
        body,
        out_shape=[jax.ShapeDtypeStruct(s, d) for s, d in outs],
        out_specs=[VM] * len(outs),
        scratch_shapes=list(scratch),
        compiler_params=pltpu.CompilerParams(vmem_limit_bytes=48 << 20),
        cost_estimate=pl.CostEstimate(flops=flops, bytes_accessed=1 << 20, transcendentals=0),
        name=name,
    )


def dot(a, b):
    return jnp.dot(a, b, preferred_element_type=F32)


def lanes(shape):
    return lax.broadcasted_iota(jnp.int32, shape, len(shape) - 1)


def roll(v, by):
    size = v.shape[-1]
    return pltpu.roll(v, by % size, v.ndim - 1)


def weights_kernel(w1, w2, w3, a1, a1s, a2, a3):
    def band(pieces, first):
        zero = jnp.zeros_like(pieces[0])
        return jnp.concatenate([zero] + pieces if first else pieces + [zero], axis=1)

    c1, c2 = w1.shape[3], w3.shape[3]
    for e in range(3):
        for f in range(3):
            p1 = [w1[a, e, f].astype(F32) for a in range(3)]
            p2 = [w2[a, e, f].astype(F32).T for a in range(3)]
            p3 = [w3[a, e, f].astype(F32) for a in range(3)]
            for xo in range(2):
                b1 = band(p1, xo).astype(BF)
                k1 = b1.shape[1]
                a1[pl.ds((xo * 3 + f) * c1, c1), pl.ds(e * k1, k1)] = b1
                a1s[pl.ds(((xo * 3 + e) * 3 + f) * c1, c1), :] = b1
                a2[pl.ds((xo * 3 + f) * c2, c2), pl.ds(e * k1, k1)] = band(p2, xo).astype(BF)
                a3[pl.ds((xo * 3 + f) * c2, c2), pl.ds(e * 2 * k1, 2 * k1)] = band(p3, xo).astype(BF)


def pack_kernel(image, own, row_a, row_b, send_a, send_b, strip_l, strip_r, lo, hi):
    chans, inline, depth, cross = image.shape
    odd = lax.axis_index("gx") % 2
    odd_y = lax.axis_index("gy") % 2
    lane = lanes((chans, 128))
    for x in range(inline):
        cells = image[:, x].astype(F32).reshape(chans * depth, cross)
        lo[...] = cells[:, :128]
        hi[...] = cells[:, cross - 128 :]
        left = jnp.zeros((chans, 128), F32)
        right = jnp.zeros((chans, 128), F32)
        for z in range(depth):
            a = lo[pl.ds(z, chans, stride=depth), :]
            b = hi[pl.ds(z, chans, stride=depth), :]
            own[z, x, :, :128] = a.astype(BF)
            own[z, x, :, 128:] = b.astype(BF)
            here = (lane >= z * G) & (lane < z * G + G)
            left = jnp.where(here, roll(a, z * G), left)
            right = jnp.where(here, roll(b, z * G + G), right)
        part = lane % G
        msg_l = jnp.where(part >= 3, roll(left, 3), 0.0).astype(BF)
        own_l = jnp.where(part >= 5, roll(left, 5), 0.0).astype(BF)
        msg_r = jnp.where(part < 5, roll(right, -3), 0.0).astype(BF)
        own_r = jnp.where(part < 3, roll(right, -5), 0.0).astype(BF)
        strip_l[x] = own_l
        strip_r[x] = own_r
        send_a[x] = jnp.where(odd_y == 0, msg_r, msg_l)
        send_b[x] = jnp.where(odd_y == 0, msg_l, msg_r)
    row_a[...] = own[:, (inline - 1) * (1 - odd)]
    row_b[...] = own[:, (inline - 1) * odd]


def strip_kernel(strip_l, strip_r, got_a, got_b, strips, corner_a, corner_b):
    inline = strip_l.shape[0]
    odd = lax.axis_index("gx") % 2
    odd_y = lax.axis_index("gy") % 2
    part = lanes(strip_l.shape) % G
    ga, gb = got_a[...], got_b[...]
    from_l = jnp.where(odd_y == 0, gb, ga)
    from_r = jnp.where(odd_y == 0, ga, gb)
    strips[:, :, :128] = jnp.where(part < 5, from_l, strip_l[...])
    strips[:, :, 128:] = jnp.where(part < 3, strip_r[...], from_r)
    corner_a[...] = strips[(inline - 1) * (1 - odd)]
    corner_b[...] = strips[(inline - 1) * odd]


def fine_pair(own, halo, halo_first, a1, bias, pooled, pad, acc):
    depth, inline, chans, cross = own.shape
    width = inline * chans
    zero = jnp.zeros((width, cross), BF)
    pad[pl.ds(0, width), :] = zero
    pad[pl.ds((depth + 1) * width, width), :] = zero
    first = 1 - halo_first

    def fill(z, carry):
        base = (z + 1) * width
        pad[pl.ds(pl.multiple_of(base + (1 - halo_first) * (inline - 1) * chans, chans), chans), :] = halo[z]
        for r in range(inline - 1):
            pad[pl.ds(pl.multiple_of(base + (r + halo_first) * chans, chans), chans), :] = own[z, first + r]
        return carry

    lax.fori_loop(0, depth, fill, 0)

    def layer(z):
        g = dot(a1[...], pad[pl.ds(pl.multiple_of(z * width, width), 3 * width), :])
        rows = []
        for xo in range(2):
            t = g[xo * 3 * chans : (xo + 1) * 3 * chans]
            rows.append(roll(t[:chans], 1) + t[chans : 2 * chans] + roll(t[2 * chans :], -1))
        return jnp.maximum(rows[0], rows[1])

    def step(z, carry):
        m = jnp.maximum(layer(2 * z), layer(2 * z + 1))
        m = jnp.maximum(jnp.maximum(m, roll(m, -1)) + bias[...], 0.0)
        acc[pl.ds(pl.multiple_of(z * chans, chans), chans), :] = m.astype(BF)
        return carry

    lax.fori_loop(0, depth // 2, step, 0)
    half = cross // 2
    src = lax.broadcasted_iota(jnp.int32, (cross, half), 0)
    dst = lax.broadcasted_iota(jnp.int32, (cross, half), 1)
    pick = jnp.where(src == 2 * dst, 1.0, 0.0).astype(BF)
    pooled[...] = dot(acc[...], pick).astype(BF).reshape(depth // 2, chans, half)


def early_kernel(own, halo, a1, bias, pooled, pad, acc):
    fine_pair(own, halo, lax.axis_index("gx") % 2, a1, bias, pooled, pad, acc)


def late_kernel(own, halo, a1, bias, pooled, pad, acc):
    fine_pair(own, halo, 1 - lax.axis_index("gx") % 2, a1, bias, pooled, pad, acc)


def edge_kernel(strips, corner_a, corner_b, early, late, a1s, bias, message, rows):
    inline, chans, _ = strips.shape
    half_depth = early.shape[0]
    odd = lax.axis_index("gx") % 2
    at = lax.axis_index("gy")
    end = lax.axis_size("gy") - 1
    ca, cb = corner_a[...], corner_b[...]
    rows[pl.ds(0, chans), :] = jnp.where(odd == 1, ca, cb)
    rows[pl.ds(chans, inline * chans), :] = strips[...].reshape(inline * chans, 256)
    rows[pl.ds((inline + 1) * chans, chans), :] = jnp.where(odd == 1, cb, ca)
    lane = lanes((chans, 128))
    for pair in range(2):
        g = dot(a1s[...], rows[pl.ds(pair * 2 * chans, 4 * chans), :])
        sides = []
        for side in range(2):
            best = None
            for xo in range(2):
                total = jnp.zeros((chans, 128), F32)
                for e in range(3):
                    part = None
                    for f in range(3):
                        k = (xo * 3 + e) * 3 + f
                        t = g[k * chans : (k + 1) * chans, side * 128 : side * 128 + 128]
                        t = roll(t, -(G * (e - 1) + f - 1))
                        part = t if part is None else part + t
                    if e == 0:
                        part = jnp.where(lane >= G, part, 0.0)
                    if e == 2:
                        part = jnp.where(lane < 128 - G, part, 0.0)
                    total = total + part
                best = total if best is None else jnp.maximum(best, total)
            best = jnp.maximum(best, roll(best, -G))
            best = jnp.maximum(best, roll(best, -1))
            best = jnp.maximum(best + bias[...], 0.0)
            cell = lane % G
            outside = (cell < 5) & (at == 0) if side == 0 else (cell > 1) & (at == end)
            sides.append(jnp.where(outside, 0.0, best))
        edges = jnp.where((lane // G) % 2 == 0, sides[0], roll(sides[1], G))
        message[pair, half_depth] = edges.astype(BF)
    message[odd, pl.ds(0, half_depth)] = late[...]
    message[1 - odd, pl.ds(0, half_depth)] = early[...]


def coarse_kernel(own, got_a, got_b, a2, b2, a3, b3, out, edge, pad2, pad3, wide):
    coarse, tall, chans, half = own.shape
    depth = tall - 1
    c2 = b2.shape[0]
    odd = lax.axis_index("gx") % 2
    at_x, end_x = lax.axis_index("gx"), lax.axis_size("gx") - 1
    at_y, end_y = lax.axis_index("gy"), lax.axis_size("gy") - 1
    width = 4 * chans
    parts = [(0, got_a, got_b), (2, None, None), (4, got_b, got_a)]

    def row_of(i, z):
        if 2 <= i < 4:
            return own[i - 2, z]
        r = i % 2
        if i < 2:
            return jnp.where(odd == 1, got_a[r, z], got_b[r, z])
        return jnp.where(odd == 1, got_b[r, z], got_a[r, z])

    src = lax.broadcasted_iota(jnp.int32, (half, 256), 0)
    dst = lax.broadcasted_iota(jnp.int32, (half, 256), 1)
    for i in range(6):
        edge[pl.ds(i * chans, chans), :] = row_of(i, depth)
    zero = jnp.zeros((width, 256), BF)
    for pair in range(2):
        pad2[pair, pl.ds(0, width), :] = zero
        pad2[pair, pl.ds((depth + 1) * width, width), :] = zero
    lane = lanes((chans, half))
    inner = (lane > 0) & (lane < half - 1)
    for z in range(depth):
        l, r = 2 * z * G, (2 * z + 1) * G
        pick = (
            ((dst == 0) & (src == l + 5))
            | ((dst == half - 1) & (src == r + 1))
            | ((dst == half) & (src == r + 3))
            | ((dst == half + 1) & (src == r + 5))
            | ((dst == 254) & (src == l + 1))
            | ((dst == 255) & (src == l + 3))
        )
        ends = dot(edge[...], jnp.where(pick, 1.0, 0.0).astype(BF)).astype(BF)
        for i in range(6):
            e = ends[i * chans : (i + 1) * chans]
            main = jnp.where(inner, row_of(i, z), e[:, :half])
            for pair in range(2):
                j = i - 2 * pair
                if 0 <= j < 4:
                    base = (z + 1) * width + j * chans
                    pad2[pair, pl.ds(base, chans), :half] = main
                    pad2[pair, pl.ds(base, chans), half:] = e[:, half:]

    wide3 = 4 * c2
    zero = jnp.zeros((wide3, 256), BF)
    pad3[pl.ds(0, wide3), :] = zero
    pad3[pl.ds((depth + 1) * wide3, wide3), :] = zero
    col = lanes((c2, 256))
    outside_y = ((col == 255) & (at_y == 0)) | ((col == half) & (at_y == end_y))

    def shifted(g):
        return roll(g[:c2], 1) + g[c2 : 2 * c2] + roll(g[2 * c2 :], -1)

    def second(z, carry):
        for pair in range(2):
            g = dot(a2[...], pad2[pair, pl.ds(pl.multiple_of(z * width, width), 3 * width), :])
            for xo in range(2):
                v = jnp.maximum(shifted(g[xo * 3 * c2 : (xo + 1) * 3 * c2]) + b2[...], 0.0)
                r = 2 * pair + xo
                outside = outside_y
                if r == 0:
                    outside = outside | (at_x == 0)
                if r == 3:
                    outside = outside | (at_x == end_x)
                v = jnp.where(outside, 0.0, v).astype(BF)
                pad3[pl.ds(pl.multiple_of((z + 1) * wide3 + r * c2, c2), c2), :] = v
        return carry

    lax.fori_loop(0, depth, second, 0)

    def third(z, carry):
        g = dot(a3[...], pad3[pl.ds(pl.multiple_of(z * wide3, wide3), 3 * wide3), :])
        for xo in range(2):
            v = jnp.maximum(shifted(g[xo * 3 * c2 : (xo + 1) * 3 * c2]) + b3[...], 0.0)
            wide[xo, pl.ds(z, c2, stride=depth), :] = v[:, :half]
        return carry

    lax.fori_loop(0, depth, third, 0)
    for xo in range(2):
        out[:, xo] = wide[xo].reshape(c2, depth, half).astype(BF)


def swap(value, axis, parity):
    pairs = []
    for i in range(parity, lax.axis_size(axis) - 1, 2):
        pairs += [(i, i + 1), (i + 1, i)]
    return lax.ppermute(value, axis, pairs)


def per_device(image, w_first, b_first, w_second, b_second, w_third, b_third):
    c1, inline, depth, cross = image.shape
    c2 = w_third.shape[0]
    half, hz = cross // 2, depth // 2
    w1 = jnp.transpose(w_first, (2, 3, 4, 0, 1))
    w2 = jnp.transpose(w_second, (2, 3, 4, 1, 0))
    w3 = jnp.transpose(w_third, (2, 3, 4, 0, 1))
    k1 = 4 * c1
    own, row_a, row_b, send_a, send_b, strip_l, strip_r = call(
        pack_kernel,
        [
            ((depth, inline, c1, cross), BF),
            ((depth, c1, cross), BF),
            ((depth, c1, cross), BF),
        ]
        + [((inline, c1, 128), BF)] * 4,
        [pltpu.VMEM((c1 * depth, 128), F32)] * 2,
        flops=1 << 20,
        name="pack",
    )(image)
    got_ya = swap(send_a, "gy", 0)
    got_yb = swap(send_b, "gy", 1)
    got_a = swap(row_a, "gx", 0)
    got_b = swap(row_b, "gx", 1)
    a1, a1s, a2, a3 = call(
        weights_kernel,
        [
            ((6 * c1, 3 * k1), BF),
            ((18 * c1, k1), BF),
            ((6 * c2, 3 * k1), BF),
            ((6 * c2, 12 * c2), BF),
        ],
        flops=1 << 28,
        name="weights",
    )(w1, w2, w3)
    b1 = b_first.reshape(c1, 1)
    b2 = b_second.reshape(c2, 1)
    b3 = b_third.reshape(c2, 1)
    strips, corner_a, corner_b = call(
        strip_kernel,
        [((inline, c1, 256), BF), ((c1, 256), BF), ((c1, 256), BF)],
        flops=1 << 20,
        name="strip",
    )(strip_l, strip_r, got_ya, got_yb)
    got_ca = swap(corner_a, "gx", 0)
    got_cb = swap(corner_b, "gx", 1)
    fine = [pltpu.VMEM(((depth + 2) * k1, cross), BF), pltpu.VMEM((hz * c1, cross), BF)]
    (early,) = call(early_kernel, [((hz, c1, half), BF)], fine, flops=1 << 30, name="early")(own, got_a, a1, b1)
    (late,) = call(late_kernel, [((hz, c1, half), BF)], fine, flops=1 << 30, name="late")(own, got_b, a1, b1)
    (message,) = call(
        edge_kernel,
        [((inline // 2, hz + 1, c1, half), BF)],
        [pltpu.VMEM(((inline + 2) * c1, 256), BF)],
        flops=1 << 28,
        name="edge",
    )(strips, got_ca, got_cb, early, late, a1s, b1)
    got_pa = swap(message, "gx", 0)
    got_pb = swap(message, "gx", 1)
    (out,) = call(
        coarse_kernel,
        [((c2, inline // 2, hz, half), BF)],
        [
            pltpu.VMEM((6 * c1, half), BF),
            pltpu.VMEM((2, (hz + 2) * k1, 256), BF),
            pltpu.VMEM(((hz + 2) * 4 * c2, 256), BF),
            pltpu.VMEM((2, c2 * hz, half), F32),
        ],
        flops=1 << 31,
        name="coarse",
    )(message, got_pa, got_pb, a2, b2, a3, b3)
    return out


def solution(mesh):
    placed = (P(None, "gx", None, "gy"), P(), P(), P(), P(), P(), P())
    return jax.shard_map(
        per_device, mesh=mesh, in_specs=placed, out_specs=P(None, "gx", None, "gy"), check_vma=False
    )
```

```python
import jax
import jax.numpy as jnp
from jax import lax
from jax.experimental import pallas as pl
from jax.experimental.pallas import tpu as pltpu
from jax.sharding import PartitionSpec as P


BF = jnp.bfloat16
F32 = jnp.float32
VM = pl.BlockSpec(memory_space=pltpu.VMEM)
G = 8


def call(body, outs, scratch=(), flops=0):
    def run(*args):
        return pl.pallas_call(
            body,
            out_shape=[jax.ShapeDtypeStruct(s, d) for s, d in outs],
            in_specs=[VM] * len(args),
            out_specs=[VM] * len(outs),
            scratch_shapes=list(scratch),
            compiler_params=pltpu.CompilerParams(vmem_limit_bytes=16 << 20),
            cost_estimate=pl.CostEstimate(flops=flops, bytes_accessed=1 << 20, transcendentals=0),
        )(*args)

    return run


def dot(a, b):
    return jnp.dot(a, b, preferred_element_type=F32)


def lanes(shape):
    return lax.broadcasted_iota(jnp.int32, shape, len(shape) - 1)


def roll(v, by):
    return pltpu.roll(v, by % v.shape[-1], v.ndim - 1)


def weights_kernel(w1, w2, w3, b1, b2, b3, a1, a1s, a2, a3, c1, c2, c3, evens, ends):
    def band(pieces, first):
        zero = jnp.zeros_like(pieces[0])
        return jnp.concatenate([zero] + pieces if first else pieces + [zero], axis=1)

    n1, n2 = w1.shape[3], w3.shape[3]
    for e in range(3):
        for f in range(3):
            p1 = [w1[a, e, f].astype(F32) for a in range(3)]
            p2 = [w2[a, e, f].astype(F32).T for a in range(3)]
            p3 = [w3[a, e, f].astype(F32) for a in range(3)]
            for xo in range(2):
                v1 = band(p1, xo).astype(BF)
                k1 = v1.shape[1]
                a1[pl.ds((xo * 3 + f) * n1, n1), pl.ds(e * k1, k1)] = v1
                a1s[pl.ds(((xo * 3 + e) * 3 + f) * n1, n1), :] = v1
                a2[pl.ds((xo * 3 + f) * n2, n2), pl.ds(e * k1, k1)] = band(p2, xo).astype(BF)
                a3[pl.ds((xo * 3 + f) * n2, n2), pl.ds(e * 2 * k1, 2 * k1)] = band(p3, xo).astype(BF)
    for b, c in ((b1, c1), (b2, c2), (b3, c3)):
        n = b.shape[1]
        eye = lax.broadcasted_iota(jnp.int32, (n, n), 0) == lax.broadcasted_iota(jnp.int32, (n, n), 1)
        column = jnp.sum(jnp.where(eye, jnp.broadcast_to(b[...], (n, n)), 0.0), axis=1, keepdims=True)
        c[...] = jnp.broadcast_to(column, c.shape)
    src = lax.broadcasted_iota(jnp.int32, evens.shape, 0)
    dst = lax.broadcasted_iota(jnp.int32, evens.shape, 1)
    evens[...] = jnp.where(src == 2 * dst, 1.0, 0.0).astype(BF)
    half = evens.shape[1]
    top = half - 2 * G
    src = lax.broadcasted_iota(jnp.int32, ends.shape, 0) - top
    dst = lax.broadcasted_iota(jnp.int32, ends.shape, 1)
    move = (
        ((dst == 0) & (src == 5))
        | ((dst == half - 1) & (src == G + 1))
        | ((dst == half) & (src == G + 3))
        | ((dst == half + 1) & (src == G + 5))
        | ((dst == 254) & (src == 1))
        | ((dst == 255) & (src == 3))
    )
    ends[...] = jnp.where(move, 1.0, 0.0).astype(BF)


def relayout(cells, lo, hi, store):
    chans, depth, cross = cells.shape
    flat = cells.astype(F32).reshape(chans * depth, cross)
    lo[...] = flat[:, :128]
    hi[...] = flat[:, 128:]
    lane = lanes((chans, 128))
    left = jnp.zeros((chans, 128), F32)
    right = jnp.zeros((chans, 128), F32)
    for z in range(depth):
        a = lo[pl.ds(z, chans, stride=depth), :]
        b = hi[pl.ds(z, chans, stride=depth), :]
        store(z, a.astype(BF), b.astype(BF))
        here = (lane >= z * G) & (lane < z * G + G)
        left = jnp.where(here, roll(a, z * G), left)
        right = jnp.where(here, roll(b, z * G + G), right)
    part = lane % G
    msg_l = jnp.where(part >= 3, roll(left, 3), 0.0).astype(BF)
    own_l = jnp.where(part >= 5, roll(left, 5), 0.0).astype(BF)
    msg_r = jnp.where(part < 5, roll(right, -3), 0.0).astype(BF)
    own_r = jnp.where(part < 3, roll(right, -5), 0.0).astype(BF)
    return msg_l, msg_r, own_l, own_r


def pack_kernel(image, own, near_row, far_row, far_small, msgs, olds, lo, hi):
    _, inline, depth, _ = image.shape
    odd = lax.axis_index("gx") % 2
    for x in range(inline):

        def store(z, a, b):
            own[z, x, :, :128] = a
            own[z, x, :, 128:] = b

        msg_l, msg_r, own_l, own_r = relayout(image[:, x], lo, hi, store)
        msgs[x, :, :128] = msg_l
        msgs[x, :, 128:] = msg_r
        olds[x, :, :128] = own_l
        olds[x, :, 128:] = own_r
    near, far = (inline - 1) * (1 - odd), (inline - 1) * odd
    near_row[pl.ds(0, depth)] = own[:, near]
    near_row[depth] = msgs[near]
    near_row[depth + 1] = olds[near]
    far_row[...] = own[:, far]
    far_small[0] = msgs[far]
    far_small[1] = olds[far]


def at_map_end():
    at = lax.axis_index("gx")
    return (at == 0) | (at == lax.axis_size("gx") - 1)


def strip_kernel(far_row, mate, msgs, olds, send_l, send_r, strips):
    inline = msgs.shape[0]
    depth = mate.shape[0] - 2
    odd = lax.axis_index("gx") % 2
    outside = at_map_end()
    far, near = (inline + 1) * odd, (inline + 1) * (1 - odd)
    zero = jnp.zeros(strips.shape[1:], BF)
    far_msg = jnp.where(outside, zero, far_row[0])
    near_msg = mate[depth]
    strips[pl.ds(1, inline)] = olds[...]
    strips[near] = mate[depth + 1]
    strips[far] = jnp.where(outside, zero, far_row[1])
    for send, half in ((send_l, pl.ds(0, 128)), (send_r, pl.ds(128, 128))):
        send[pl.ds(1, inline)] = msgs[:, :, half]
        send[near] = near_msg[:, half.start : half.start + 128]
        send[far] = far_msg[:, half.start : half.start + 128]


def fine_pair(own, halo, halo_first, outside, a1, bias, evens, pooled, pad, acc):
    depth, inline, chans, cross = own.shape
    width = inline * chans
    zero = jnp.zeros((width, cross), BF)
    pad[pl.ds(0, width), :] = zero
    pad[pl.ds((depth + 1) * width, width), :] = zero
    first = 1 - halo_first
    for z in range(depth):
        base = (z + 1) * width
        beyond = halo[z] if outside is None else jnp.where(outside, zero[:chans], halo[z])
        pad[pl.ds(pl.multiple_of(base + (1 - halo_first) * (inline - 1) * chans, chans), chans), :] = beyond
        for r in range(inline - 1):
            pad[pl.ds(pl.multiple_of(base + (r + halo_first) * chans, chans), chans), :] = own[z, first + r]

    def layer(z):
        g = dot(a1[...], pad[pl.ds(z * width, 3 * width), :])
        rows = []
        for xo in range(2):
            t = g[xo * 3 * chans : (xo + 1) * 3 * chans]
            rows.append(roll(t[:chans], 1) + t[chans : 2 * chans] + roll(t[2 * chans :], -1))
        return jnp.maximum(rows[0], rows[1])

    for z in range(depth // 2):
        m = jnp.maximum(layer(2 * z), layer(2 * z + 1))
        m = jnp.maximum(jnp.maximum(m, roll(m, -1)) + bias[...], 0.0)
        acc[pl.ds(z * chans, chans), :] = m.astype(BF)
    pooled[...] = dot(acc[...], evens[...]).astype(BF).reshape(pooled.shape)


def early_kernel(own, mate, a1, bias, evens, pooled, pad, acc):
    fine_pair(own, mate, lax.axis_index("gx") % 2, None, a1, bias, evens, pooled, pad, acc)


def late_kernel(own, halo, strips, got_l, got_r, early, a1, a1s, bias, evens, message, pad, acc, rows, late):
    tall, chans, _ = strips.shape
    half_depth = early.shape[0]
    odd = lax.axis_index("gx") % 2
    message[1 - odd, pl.ds(0, half_depth)] = early[...]
    fine_pair(own, halo, 1 - odd, at_map_end(), a1, bias, evens, late, pad, acc)
    message[odd, pl.ds(0, half_depth)] = late[...]
    at, end = lax.axis_index("gy"), lax.axis_size("gy") - 1
    part = lanes((tall * chans, 128)) % G
    from_l = jnp.where(at == 0, 0.0, got_l[...].reshape(tall * chans, 128))
    from_r = jnp.where(at == end, 0.0, got_r[...].reshape(tall * chans, 128))
    s = strips[...].reshape(tall * chans, 256)
    rows[:, :128] = jnp.where(part < 5, from_l, s[:, :128]).astype(BF)
    rows[:, 128:] = jnp.where(part < 3, s[:, 128:], from_r).astype(BF)
    lane = lanes((chans, 128))
    for pair in range(2):
        g = dot(a1s[...], rows[pl.ds(pair * 2 * chans, 4 * chans), :])
        sides = []
        for side in range(2):
            best = None
            for xo in range(2):
                total = None
                for e in range(3):
                    part = None
                    for f in range(3):
                        k = (xo * 3 + e) * 3 + f
                        t = g[k * chans : (k + 1) * chans, side * 128 : side * 128 + 128]
                        t = roll(t, -(G * (e - 1) + f - 1))
                        part = t if part is None else part + t
                    if e == 0:
                        part = jnp.where(lane >= G, part, 0.0)
                    if e == 2:
                        part = jnp.where(lane < 128 - G, part, 0.0)
                    total = part if total is None else total + part
                best = total if best is None else jnp.maximum(best, total)
            best = jnp.maximum(best, roll(best, -G))
            best = jnp.maximum(best, roll(best, -1))
            best = jnp.maximum(best + bias[:, :128], 0.0)
            cell = lane % G
            outside = (cell < 5) & (at == 0) if side == 0 else (cell > 1) & (at == end)
            sides.append(jnp.where(outside, 0.0, best))
        edges = jnp.where((lane // G) % 2 == 0, sides[0], roll(sides[1], G))
        message[pair, half_depth] = edges.astype(BF)


def coarse_pair(own, other, own_first, beyond, a2, bias, ends, outside_x, put, pad, edge):
    coarse, tall, chans, half = own.shape
    depth = tall - 1
    c2 = bias.shape[0]
    width = 2 * coarse * chans
    at, end = lax.axis_index("gy"), lax.axis_size("gy") - 1
    spots = [(1 - own_first) * coarse, own_first * coarse]
    for source, spot in zip((own, other), spots):
        for r in range(coarse):
            value = source[r, depth]
            if source is other and beyond is not None:
                value = jnp.where(beyond, jnp.zeros_like(value), value)
            edge[pl.ds(pl.multiple_of((spot + r) * chans, chans), chans), :] = value
    zero = jnp.zeros((width, 256), BF)
    pad[pl.ds(0, width), :] = zero
    pad[pl.ds((depth + 1) * width, width), :] = zero
    lane = lanes((chans, half))
    inner = (lane > 0) & (lane < half - 1)
    for z in range(depth):
        base = (z + 1) * width
        fixed = dot(edge[...], ends[pl.ds(half - 2 * G - 2 * G * z, half), :]).astype(BF)
        pad[pl.ds(base, width), :] = fixed
        for source, spot in zip((own, other), spots):
            for r in range(coarse):
                where = pl.ds(pl.multiple_of(base + (spot + r) * chans, chans), chans)
                use = inner if source is own or beyond is None else inner & ~beyond
                pad[where, :half] = jnp.where(use, source[r, z], pad[where, :half])
    col = lanes((c2, 256))
    outside_y = ((col == 255) & (at == 0)) | ((col == half) & (at == end))
    for z in range(depth):
        g = dot(a2[...], pad[pl.ds(z * width, 3 * width), :])
        for xo in range(2):
            t = g[xo * 3 * c2 : (xo + 1) * 3 * c2]
            v = roll(t[:c2], 1) + t[c2 : 2 * c2] + roll(t[2 * c2 :], -1)
            v = jnp.maximum(v + bias[...], 0.0)
            hide = outside_y if outside_x is None else outside_y | outside_x[xo]
            put(z, xo, jnp.where(hide, 0.0, v).astype(BF))


def coarse_early_kernel(own, mate, a2, bias, ends, second, pad, edge):
    def put(z, xo, v):
        second[z, xo] = v

    coarse_pair(own, mate, 1 - lax.axis_index("gx") % 2, None, a2, bias, ends, None, put, pad, edge)


def coarse_late_kernel(own, far, second, a2, b2, a3, b3, ends, out, pad, edge, pad3, wide):
    depth, _, c2, _ = second.shape
    half = out.shape[-1]
    odd = lax.axis_index("gx") % 2
    at, end = lax.axis_index("gx"), lax.axis_size("gx") - 1
    width = 4 * c2
    zero = jnp.zeros((width, 256), BF)
    pad3[pl.ds(0, width), :] = zero
    pad3[pl.ds((depth + 1) * width, width), :] = zero
    for z in range(depth):
        for r in range(2):
            spot = (z + 1) * width + ((1 - odd) * 2 + r) * c2
            pad3[pl.ds(pl.multiple_of(spot, c2), c2), :] = second[z, r]

    def put(z, xo, v):
        spot = (z + 1) * width + (odd * 2 + xo) * c2
        pad3[pl.ds(pl.multiple_of(spot, c2), c2), :] = v

    outside = [(odd == 0) & (at == 0), (odd == 1) & (at == end)]
    coarse_pair(own, far, odd, at_map_end(), a2, b2, ends, outside, put, pad, edge)
    for z in range(depth):
        g = dot(a3[...], pad3[pl.ds(z * width, 3 * width), :])
        for xo in range(2):
            t = g[xo * 3 * c2 : (xo + 1) * 3 * c2]
            v = roll(t[:c2], 1) + t[c2 : 2 * c2] + roll(t[2 * c2 :], -1)
            v = jnp.maximum(v + b3[...], 0.0)
            wide[xo, pl.ds(z, c2, stride=depth), :] = v[:, :half]
    for xo in range(2):
        out[:, xo] = wide[xo].reshape(c2, depth, half).astype(BF)


def swap(value, parity):
    count = lax.axis_size("gx")
    pairs = []
    for i in range(parity, count, 2):
        j = (i + 1) % count
        pairs += [(i, j), (j, i)]
    return lax.ppermute(value, "gx", pairs)


def shift(value, by):
    count = lax.axis_size("gy")
    return lax.ppermute(value, "gy", [(i, (i + by) % count) for i in range(count)])


def per_device(image, w_first, b_first, w_second, b_second, w_third, b_third):
    c1, inline, depth, cross = image.shape
    c2 = w_third.shape[0]
    half, hz, coarse = cross // 2, depth // 2, inline // 2
    k1 = 4 * c1
    tall = inline + 2
    own, near_row, far_row, far_small, msgs, olds = call(
        pack_kernel,
        [
            ((depth, inline, c1, cross), BF),
            ((depth + 2, c1, cross), BF),
            ((depth, c1, cross), BF),
            ((2, c1, 256), BF),
            ((inline, c1, 256), BF),
            ((inline, c1, 256), BF),
        ],
        scratch=[pltpu.VMEM((c1 * depth, 128), F32)] * 2,
        flops=1 << 28,
    )(image)
    got_small = swap(far_small, 1)
    got_far = swap(far_row, 1)
    got_row = swap(near_row, 0)
    a1, a1s, a2, a3, b1, b2, b3, evens, ends = call(
        weights_kernel,
        [
            ((6 * c1, 3 * k1), BF),
            ((18 * c1, k1), BF),
            ((6 * c2, 3 * k1), BF),
            ((6 * c2, 12 * c2), BF),
            ((c1, 256), F32),
            ((c2, 256), F32),
            ((c2, 256), F32),
            ((cross, half), BF),
            ((2 * half, 256), BF),
        ],
        flops=1 << 28,
    )(
        jnp.transpose(w_first, (2, 3, 4, 0, 1)),
        jnp.transpose(w_second, (2, 3, 4, 1, 0)),
        jnp.transpose(w_third, (2, 3, 4, 0, 1)),
        b_first.reshape(1, c1),
        b_second.reshape(1, c2),
        b_third.reshape(1, c2),
    )
    fine = [pltpu.VMEM(((depth + 2) * k1, cross), BF), pltpu.VMEM((hz * c1, cross), BF)]
    (early,) = call(early_kernel, [((hz, c1, half), BF)], scratch=fine, flops=1 << 29)(own, got_row, a1, b1, evens)
    send_l, send_r, strips = call(
        strip_kernel, [((tall, c1, 128), BF)] * 2 + [((tall, c1, 256), BF)], flops=1 << 20
    )(got_small, got_row, msgs, olds)
    got_l = shift(send_r, 1)
    got_r = shift(send_l, -1)
    (message,) = call(
        late_kernel,
        [((coarse, hz + 1, c1, half), BF)],
        scratch=fine + [pltpu.VMEM((tall * c1, 256), BF), pltpu.VMEM((hz, c1, half), BF)],
        flops=1 << 29,
    )(own, got_far, strips, got_l, got_r, early, a1, a1s, b1, evens)
    got_pa = swap(message, 0)
    got_pb = swap(message, 1)
    mid = [pltpu.VMEM(((hz + 2) * k1, 256), BF), pltpu.VMEM((k1, half), BF)]
    (second,) = call(
        coarse_early_kernel, [((hz, 2, c2, 256), BF)], scratch=mid, flops=1 << 29
    )(message, got_pa, a2, b2, ends)
    (out,) = call(
        coarse_late_kernel,
        [((c2, coarse, hz, half), BF)],
        scratch=mid + [pltpu.VMEM(((hz + 2) * 4 * c2, 256), BF), pltpu.VMEM((coarse, c2 * hz, half), F32)],
        flops=1 << 29,
    )(message, got_pb, second, a2, b2, a3, b3, ends)
    return out


def solution(mesh):
    placed = (P(None, "gx", None, "gy"), P(), P(), P(), P(), P(), P())

    return jax.shard_map(per_device, mesh=mesh, in_specs=placed, out_specs=P(None, "gx", None, "gy"), check_vma=False)
```

```python
import jax
import jax.numpy as jnp
from jax import lax
from jax.experimental import pallas as pl
from jax.experimental.pallas import tpu as pltpu
from jax.sharding import PartitionSpec as P


BF = jnp.bfloat16
F32 = jnp.float32
VM = pl.BlockSpec(memory_space=pltpu.VMEM)
G = 8


def call(body, outs, scratch=(), flops=0):
    def run(*args):
        return pl.pallas_call(
            body,
            out_shape=[jax.ShapeDtypeStruct(s, d) for s, d in outs],
            in_specs=[VM] * len(args),
            out_specs=[VM] * len(outs),
            scratch_shapes=list(scratch),
            compiler_params=pltpu.CompilerParams(vmem_limit_bytes=16 << 20),
            cost_estimate=pl.CostEstimate(flops=flops, bytes_accessed=1 << 20, transcendentals=0),
        )(*args)

    return run


def dot(a, b):
    return jnp.dot(a, b, preferred_element_type=F32)


def lanes(shape):
    return lax.broadcasted_iota(jnp.int32, shape, len(shape) - 1)


def roll(v, by):
    return pltpu.roll(v, by % v.shape[-1], v.ndim - 1)


def weights_kernel(w1, w2, w3, b1, b2, b3, a1, a1s, a2, a3, c1, c2, c3, evens, ends):
    def band(pieces, first):
        zero = jnp.zeros_like(pieces[0])
        return jnp.concatenate([zero] + pieces if first else pieces + [zero], axis=1)

    n1, n2 = w1.shape[3], w3.shape[3]
    for e in range(3):
        for f in range(3):
            p1 = [w1[a, e, f].astype(F32) for a in range(3)]
            p2 = [w2[a, e, f].astype(F32).T for a in range(3)]
            p3 = [w3[a, e, f].astype(F32) for a in range(3)]
            for xo in range(2):
                v1 = band(p1, xo).astype(BF)
                k1 = v1.shape[1]
                a1[pl.ds((xo * 3 + f) * n1, n1), pl.ds(e * k1, k1)] = v1
                a1s[pl.ds(((xo * 3 + e) * 3 + f) * n1, n1), :] = v1
                a2[pl.ds((xo * 3 + f) * n2, n2), pl.ds(e * k1, k1)] = band(p2, xo).astype(BF)
                a3[pl.ds((xo * 3 + f) * n2, n2), pl.ds(e * 2 * k1, 2 * k1)] = band(p3, xo).astype(BF)
    for b, c in ((b1, c1), (b2, c2), (b3, c3)):
        n = b.shape[1]
        eye = lax.broadcasted_iota(jnp.int32, (n, n), 0) == lax.broadcasted_iota(jnp.int32, (n, n), 1)
        column = jnp.sum(jnp.where(eye, jnp.broadcast_to(b[...], (n, n)), 0.0), axis=1, keepdims=True)
        c[...] = jnp.broadcast_to(column, c.shape)
    src = lax.broadcasted_iota(jnp.int32, evens.shape, 0)
    dst = lax.broadcasted_iota(jnp.int32, evens.shape, 1)
    evens[...] = jnp.where(src == 2 * dst, 1.0, 0.0).astype(BF)
    half = evens.shape[1]
    top = half - 2 * G
    src = lax.broadcasted_iota(jnp.int32, ends.shape, 0) - top
    dst = lax.broadcasted_iota(jnp.int32, ends.shape, 1)
    move = (
        ((dst == 0) & (src == 5))
        | ((dst == half - 1) & (src == G + 1))
        | ((dst == half) & (src == G + 3))
        | ((dst == half + 1) & (src == G + 5))
        | ((dst == 254) & (src == 1))
        | ((dst == 255) & (src == 3))
    )
    ends[...] = jnp.where(move, 1.0, 0.0).astype(BF)


def relayout(cells, lo, hi, store):
    chans, depth, cross = cells.shape
    flat = cells.astype(F32).reshape(chans * depth, cross)
    lo[...] = flat[:, :128]
    hi[...] = flat[:, 128:]
    lane = lanes((chans, 128))
    left = jnp.zeros((chans, 128), F32)
    right = jnp.zeros((chans, 128), F32)
    for z in range(depth):
        a = lo[pl.ds(z, chans, stride=depth), :]
        b = hi[pl.ds(z, chans, stride=depth), :]
        store(z, a.astype(BF), b.astype(BF))
        here = (lane >= z * G) & (lane < z * G + G)
        left = jnp.where(here, roll(a, z * G), left)
        right = jnp.where(here, roll(b, z * G + G), right)
    part = lane % G
    msg_l = jnp.where(part >= 3, roll(left, 3), 0.0).astype(BF)
    own_l = jnp.where(part >= 5, roll(left, 5), 0.0).astype(BF)
    msg_r = jnp.where(part < 5, roll(right, -3), 0.0).astype(BF)
    own_r = jnp.where(part < 3, roll(right, -5), 0.0).astype(BF)
    return msg_l, msg_r, own_l, own_r


def pack_kernel(image, own, near_row, far_row, far_small, msgs, olds, lo, hi):
    _, inline, depth, _ = image.shape
    odd = lax.axis_index("gx") % 2
    for x in range(inline):

        def store(z, a, b):
            own[z, x, :, :128] = a
            own[z, x, :, 128:] = b

        msg_l, msg_r, own_l, own_r = relayout(image[:, x], lo, hi, store)
        msgs[x, :, :128] = msg_l
        msgs[x, :, 128:] = msg_r
        olds[x, :, :128] = own_l
        olds[x, :, 128:] = own_r
    near, far = (inline - 1) * (1 - odd), (inline - 1) * odd
    near_row[pl.ds(0, depth)] = own[:, near]
    near_row[depth] = msgs[near]
    near_row[depth + 1] = olds[near]
    far_row[...] = own[:, far]
    far_small[0] = msgs[far]
    far_small[1] = olds[far]


def at_map_end():
    at = lax.axis_index("gx")
    return (at == 0) | (at == lax.axis_size("gx") - 1)


def strip_kernel(far_row, mate, msgs, olds, send_1, send_2, strips):
    inline = msgs.shape[0]
    depth = mate.shape[0] - 2
    odd = lax.axis_index("gx") % 2
    outside = at_map_end()
    far, near = (inline + 1) * odd, (inline + 1) * (1 - odd)
    zero = jnp.zeros(strips.shape[1:], BF)
    far_msg = jnp.where(outside, zero, far_row[0])
    near_msg = mate[depth]
    strips[pl.ds(1, inline)] = olds[...]
    strips[near] = mate[depth + 1]
    strips[far] = jnp.where(outside, zero, far_row[1])
    for send, right in ((send_1, odd == 0), (send_2, odd == 1)):

        def pick(v):
            return jnp.where(right, v[..., 128:], v[..., :128])

        send[pl.ds(1, inline)] = pick(msgs[...])
        send[near] = pick(near_msg)
        send[far] = pick(far_msg)


def fine_pair(own, halo, halo_first, outside, a1, bias, evens, pooled, pad, acc):
    depth, inline, chans, cross = own.shape
    width = inline * chans
    zero = jnp.zeros((width, cross), BF)
    pad[pl.ds(0, width), :] = zero
    pad[pl.ds((depth + 1) * width, width), :] = zero
    first = 1 - halo_first
    for z in range(depth):
        base = (z + 1) * width
        beyond = halo[z] if outside is None else jnp.where(outside, zero[:chans], halo[z])
        pad[pl.ds(pl.multiple_of(base + (1 - halo_first) * (inline - 1) * chans, chans), chans), :] = beyond
        for r in range(inline - 1):
            pad[pl.ds(pl.multiple_of(base + (r + halo_first) * chans, chans), chans), :] = own[z, first + r]

    def layer(z):
        g = dot(a1[...], pad[pl.ds(z * width, 3 * width), :])
        rows = []
        for xo in range(2):
            t = g[xo * 3 * chans : (xo + 1) * 3 * chans]
            rows.append(roll(t[:chans], 1) + t[chans : 2 * chans] + roll(t[2 * chans :], -1))
        return jnp.maximum(rows[0], rows[1])

    for z in range(depth // 2):
        m = jnp.maximum(layer(2 * z), layer(2 * z + 1))
        m = jnp.maximum(jnp.maximum(m, roll(m, -1)) + bias[...], 0.0)
        acc[pl.ds(z * chans, chans), :] = m.astype(BF)
    pooled[...] = dot(acc[...], evens[...]).astype(BF).reshape(pooled.shape)


def early_kernel(own, mate, a1, bias, evens, pooled, pad, acc):
    fine_pair(own, mate, lax.axis_index("gx") % 2, None, a1, bias, evens, pooled, pad, acc)


def late_kernel(own, halo, strips, got_1, got_2, early, a1, a1s, bias, evens, message, pad, acc, rows, late):
    tall, chans, _ = strips.shape
    half_depth = early.shape[0]
    odd = lax.axis_index("gx") % 2
    message[1 - odd, pl.ds(0, half_depth)] = early[...]
    fine_pair(own, halo, 1 - odd, at_map_end(), a1, bias, evens, late, pad, acc)
    message[odd, pl.ds(0, half_depth)] = late[...]
    at, end = lax.axis_index("gy"), lax.axis_size("gy") - 1
    part = lanes((tall * chans, 128)) % G
    one, two = got_1[...].reshape(tall * chans, 128), got_2[...].reshape(tall * chans, 128)
    from_l = jnp.where(at == 0, 0.0, jnp.where(odd == 0, one, two))
    from_r = jnp.where(at == end, 0.0, jnp.where(odd == 0, two, one))
    s = strips[...].reshape(tall * chans, 256)
    rows[:, :128] = jnp.where(part < 5, from_l, s[:, :128]).astype(BF)
    rows[:, 128:] = jnp.where(part < 3, s[:, 128:], from_r).astype(BF)
    lane = lanes((chans, 128))
    for pair in range(2):
        g = dot(a1s[...], rows[pl.ds(pair * 2 * chans, 4 * chans), :])
        sides = []
        for side in range(2):
            best = None
            for xo in range(2):
                total = None
                for e in range(3):
                    part = None
                    for f in range(3):
                        k = (xo * 3 + e) * 3 + f
                        t = g[k * chans : (k + 1) * chans, side * 128 : side * 128 + 128]
                        t = roll(t, -(G * (e - 1) + f - 1))
                        part = t if part is None else part + t
                    if e == 0:
                        part = jnp.where(lane >= G, part, 0.0)
                    if e == 2:
                        part = jnp.where(lane < 128 - G, part, 0.0)
                    total = part if total is None else total + part
                best = total if best is None else jnp.maximum(best, total)
            best = jnp.maximum(best, roll(best, -G))
            best = jnp.maximum(best, roll(best, -1))
            best = jnp.maximum(best + bias[:, :128], 0.0)
            cell = lane % G
            outside = (cell < 5) & (at == 0) if side == 0 else (cell > 1) & (at == end)
            sides.append(jnp.where(outside, 0.0, best))
        edges = jnp.where((lane // G) % 2 == 0, sides[0], roll(sides[1], G))
        message[pair, half_depth] = edges.astype(BF)


def coarse_pair(own, other, own_first, beyond, a2, bias, ends, outside_x, put, pad, edge):
    coarse, tall, chans, half = own.shape
    depth = tall - 1
    c2 = bias.shape[0]
    width = 2 * coarse * chans
    at, end = lax.axis_index("gy"), lax.axis_size("gy") - 1
    spots = [(1 - own_first) * coarse, own_first * coarse]
    for source, spot in zip((own, other), spots):
        for r in range(coarse):
            value = source[r, depth]
            if source is other and beyond is not None:
                value = jnp.where(beyond, jnp.zeros_like(value), value)
            edge[pl.ds(pl.multiple_of((spot + r) * chans, chans), chans), :] = value
    zero = jnp.zeros((width, 256), BF)
    pad[pl.ds(0, width), :] = zero
    pad[pl.ds((depth + 1) * width, width), :] = zero
    lane = lanes((chans, half))
    inner = (lane > 0) & (lane < half - 1)
    for z in range(depth):
        base = (z + 1) * width
        fixed = dot(edge[...], ends[pl.ds(half - 2 * G - 2 * G * z, half), :]).astype(BF)
        pad[pl.ds(base, width), :] = fixed
        for source, spot in zip((own, other), spots):
            for r in range(coarse):
                where = pl.ds(pl.multiple_of(base + (spot + r) * chans, chans), chans)
                use = inner if source is own or beyond is None else inner & ~beyond
                pad[where, :half] = jnp.where(use, source[r, z], pad[where, :half])
    col = lanes((c2, 256))
    outside_y = ((col == 255) & (at == 0)) | ((col == half) & (at == end))
    for z in range(depth):
        g = dot(a2[...], pad[pl.ds(z * width, 3 * width), :])
        for xo in range(2):
            t = g[xo * 3 * c2 : (xo + 1) * 3 * c2]
            v = roll(t[:c2], 1) + t[c2 : 2 * c2] + roll(t[2 * c2 :], -1)
            v = jnp.maximum(v + bias[...], 0.0)
            hide = outside_y if outside_x is None else outside_y | outside_x[xo]
            put(z, xo, jnp.where(hide, 0.0, v).astype(BF))


def coarse_early_kernel(own, mate, a2, bias, ends, second, pad, edge):
    def put(z, xo, v):
        second[z, xo] = v

    coarse_pair(own, mate, 1 - lax.axis_index("gx") % 2, None, a2, bias, ends, None, put, pad, edge)


def coarse_late_kernel(own, far, second, a2, b2, a3, b3, ends, out, pad, edge, pad3, wide):
    depth, _, c2, _ = second.shape
    half = out.shape[-1]
    odd = lax.axis_index("gx") % 2
    at, end = lax.axis_index("gx"), lax.axis_size("gx") - 1
    width = 4 * c2
    zero = jnp.zeros((width, 256), BF)
    pad3[pl.ds(0, width), :] = zero
    pad3[pl.ds((depth + 1) * width, width), :] = zero
    for z in range(depth):
        for r in range(2):
            spot = (z + 1) * width + ((1 - odd) * 2 + r) * c2
            pad3[pl.ds(pl.multiple_of(spot, c2), c2), :] = second[z, r]

    def put(z, xo, v):
        spot = (z + 1) * width + (odd * 2 + xo) * c2
        pad3[pl.ds(pl.multiple_of(spot, c2), c2), :] = v

    outside = [(odd == 0) & (at == 0), (odd == 1) & (at == end)]
    coarse_pair(own, far, odd, at_map_end(), a2, b2, ends, outside, put, pad, edge)
    for z in range(depth):
        g = dot(a3[...], pad3[pl.ds(z * width, 3 * width), :])
        for xo in range(2):
            t = g[xo * 3 * c2 : (xo + 1) * 3 * c2]
            v = roll(t[:c2], 1) + t[c2 : 2 * c2] + roll(t[2 * c2 :], -1)
            v = jnp.maximum(v + b3[...], 0.0)
            wide[xo, pl.ds(z, c2, stride=depth), :] = v[:, :half]
    for xo in range(2):
        out[:, xo] = wide[xo].reshape(c2, depth, half).astype(BF)


def permute(value, target):
    wide, deep = lax.axis_size("gx"), lax.axis_size("gy")
    pairs = []
    for x in range(wide):
        for y in range(deep):
            tx, ty = target(x, y, wide, deep)
            pairs.append((x * deep + y, tx * deep + ty))
    return lax.ppermute(value, ("gx", "gy"), pairs)


def mate_of(x, y, wide, deep):
    return x ^ 1, y


def far_of(x, y, wide, deep):
    to = x + 1 if x % 2 else x - 1
    if 0 <= to < wide:
        return to, y
    if deep % 2 == 0:
        return x, y ^ 1
    return to % wide, y


def loop_of(up):
    def target(x, y, wide, deep):
        to = y + 1 if (x % 2 == 0) == up else y - 1
        return (x, to) if 0 <= to < deep else (x ^ 1, y)

    return target


def per_device(image, w_first, b_first, w_second, b_second, w_third, b_third):
    c1, inline, depth, cross = image.shape
    c2 = w_third.shape[0]
    half, hz, coarse = cross // 2, depth // 2, inline // 2
    k1 = 4 * c1
    tall = inline + 2
    own, near_row, far_row, far_small, msgs, olds = call(
        pack_kernel,
        [
            ((depth, inline, c1, cross), BF),
            ((depth + 2, c1, cross), BF),
            ((depth, c1, cross), BF),
            ((2, c1, 256), BF),
            ((inline, c1, 256), BF),
            ((inline, c1, 256), BF),
        ],
        scratch=[pltpu.VMEM((c1 * depth, 128), F32)] * 2,
        flops=1 << 28,
    )(image)
    got_small = permute(far_small, far_of)
    got_far = permute(far_row, far_of)
    got_row = permute(near_row, mate_of)
    a1, a1s, a2, a3, b1, b2, b3, evens, ends = call(
        weights_kernel,
        [
            ((6 * c1, 3 * k1), BF),
            ((18 * c1, k1), BF),
            ((6 * c2, 3 * k1), BF),
            ((6 * c2, 12 * c2), BF),
            ((c1, 256), F32),
            ((c2, 256), F32),
            ((c2, 256), F32),
            ((cross, half), BF),
            ((2 * half, 256), BF),
        ],
        flops=1 << 28,
    )(
        jnp.transpose(w_first, (2, 3, 4, 0, 1)),
        jnp.transpose(w_second, (2, 3, 4, 1, 0)),
        jnp.transpose(w_third, (2, 3, 4, 0, 1)),
        b_first.reshape(1, c1),
        b_second.reshape(1, c2),
        b_third.reshape(1, c2),
    )
    fine = [pltpu.VMEM(((depth + 2) * k1, cross), BF), pltpu.VMEM((hz * c1, cross), BF)]
    (early,) = call(early_kernel, [((hz, c1, half), BF)], scratch=fine, flops=1 << 29)(own, got_row, a1, b1, evens)
    send_1, send_2, strips = call(
        strip_kernel, [((tall, c1, 128), BF)] * 2 + [((tall, c1, 256), BF)], flops=1 << 20
    )(got_small, got_row, msgs, olds)
    got_1 = permute(send_1, loop_of(True))
    got_2 = permute(send_2, loop_of(False))
    (message,) = call(
        late_kernel,
        [((coarse, hz + 1, c1, half), BF)],
        scratch=fine + [pltpu.VMEM((tall * c1, 256), BF), pltpu.VMEM((hz, c1, half), BF)],
        flops=1 << 29,
    )(own, got_far, strips, got_1, got_2, early, a1, a1s, b1, evens)
    got_pa = permute(message, mate_of)
    got_pb = permute(message, far_of)
    mid = [pltpu.VMEM(((hz + 2) * k1, 256), BF), pltpu.VMEM((k1, half), BF)]
    (second,) = call(
        coarse_early_kernel, [((hz, 2, c2, 256), BF)], scratch=mid, flops=1 << 29
    )(message, got_pa, a2, b2, ends)
    (out,) = call(
        coarse_late_kernel,
        [((c2, coarse, hz, half), BF)],
        scratch=mid + [pltpu.VMEM(((hz + 2) * 4 * c2, 256), BF), pltpu.VMEM((coarse, c2 * hz, half), F32)],
        flops=1 << 29,
    )(message, got_pb, second, a2, b2, a3, b3, ends)
    return out


def solution(mesh):
    placed = (P(None, "gx", None, "gy"), P(), P(), P(), P(), P(), P())

    return jax.shard_map(per_device, mesh=mesh, in_specs=placed, out_specs=P(None, "gx", None, "gy"), check_vma=False)
```

```python
import jax
import jax.numpy as jnp
from jax import lax
from jax.experimental import pallas as pl
from jax.experimental.pallas import tpu as pltpu
from jax.sharding import PartitionSpec as P


BF = jnp.bfloat16
F32 = jnp.float32
VM = pl.BlockSpec(memory_space=pltpu.VMEM)
G = 8


def call(body, outs, scratch=(), flops=0):
    def run(*args):
        return pl.pallas_call(
            body,
            out_shape=[jax.ShapeDtypeStruct(s, d) for s, d in outs],
            in_specs=[VM] * len(args),
            out_specs=[VM] * len(outs),
            scratch_shapes=list(scratch),
            compiler_params=pltpu.CompilerParams(vmem_limit_bytes=16 << 20),
            cost_estimate=pl.CostEstimate(flops=flops, bytes_accessed=1 << 20, transcendentals=0),
        )(*args)

    return run


def dot(a, b):
    return jnp.dot(a, b, preferred_element_type=F32)


def lanes(shape):
    return lax.broadcasted_iota(jnp.int32, shape, len(shape) - 1)


def roll(v, by):
    return pltpu.roll(v, by % v.shape[-1], v.ndim - 1)


def weights_kernel(w1, w2, w3, b1, b2, b3, a1, a1s, a1h, a2, a3, c1, c2, c3, evens, ends):
    n1, n2 = w1.shape[3], w3.shape[3]
    zero1, zero3 = jnp.zeros((n1, n1), F32), jnp.zeros((n2, n2), F32)
    zero2 = jnp.zeros((n2, n1), F32)
    p1, p2, p3 = {}, {}, {}
    for e in range(3):
        for f in range(3):
            for a in range(-1, 4):
                inside = 0 <= a < 3
                p1[a, e, f] = w1[a, e, f].astype(F32) if inside else zero1
                p2[a, e, f] = w2[a, e, f].astype(F32).T if inside else zero2
                p3[a, e, f] = w3[a, e, f].astype(F32) if inside else zero3
    join = lambda pieces: jnp.concatenate(pieces, axis=1).astype(BF)
    for xo in range(2):
        for f in range(3):
            for e in range(3):
                v = join([p1[xi - xo, e, f] for xi in range(4)])
                a1[pl.ds((xo * 3 + f) * n1, n1), pl.ds(e * 4 * n1, 4 * n1)] = v
                a1s[pl.ds(((xo * 3 + e) * 3 + f) * n1, n1), :] = v
            for h in range(2):
                row = [p2[2 * h + r - xo, e, f] for e in range(3) for r in range(2)]
                a2[h, pl.ds((xo * 3 + f) * n2, n2), :] = join(row)
                for e in range(3):
                    spot = pl.ds((e * 3 + f) * 2 * n2, 2 * n2)
                    a3[h, pl.ds(xo * n2, n2), spot] = join([p3[2 * h + r - xo, e, f] for r in range(2)])
    for h in range(2):
        for f in range(3):
            a1h[h, pl.ds(f * n1, n1), :] = join([p1[2 * h, e, f] for e in range(3)])
    for b, c in ((b1, c1), (b2, c2), (b3, c3)):
        n = b.shape[1]
        eye = lax.broadcasted_iota(jnp.int32, (n, n), 0) == lax.broadcasted_iota(jnp.int32, (n, n), 1)
        column = jnp.sum(jnp.where(eye, jnp.broadcast_to(b[...], (n, n)), 0.0), axis=1, keepdims=True)
        c[...] = jnp.broadcast_to(column, c.shape)
    src = lax.broadcasted_iota(jnp.int32, evens.shape, 0)
    dst = lax.broadcasted_iota(jnp.int32, evens.shape, 1)
    evens[...] = jnp.where(src == 2 * dst, 1.0, 0.0).astype(BF)
    half = evens.shape[1]
    top = half - 2 * G
    src = lax.broadcasted_iota(jnp.int32, ends.shape, 0) - top
    dst = lax.broadcasted_iota(jnp.int32, ends.shape, 1)
    move = (
        ((dst == 0) & (src == 5))
        | ((dst == half - 1) & (src == G + 1))
        | ((dst == half) & (src == G + 3))
        | ((dst == half + 1) & (src == G + 5))
        | ((dst == 254) & (src == 1))
        | ((dst == 255) & (src == 3))
    )
    ends[...] = jnp.where(move, 1.0, 0.0).astype(BF)


def relayout(cells, lo, hi, store):
    chans, depth, cross = cells.shape
    flat = cells.astype(F32).reshape(chans * depth, cross)
    lo[...] = flat[:, :128]
    hi[...] = flat[:, 128:]
    lane = lanes((chans, 128))
    left = jnp.zeros((chans, 128), F32)
    right = jnp.zeros((chans, 128), F32)
    for z in range(depth):
        a = lo[pl.ds(z, chans, stride=depth), :]
        b = hi[pl.ds(z, chans, stride=depth), :]
        store(z, a.astype(BF), b.astype(BF))
        here = (lane >= z * G) & (lane < z * G + G)
        left = jnp.where(here, roll(a, z * G), left)
        right = jnp.where(here, roll(b, z * G + G), right)
    part = lane % G
    msg_l = jnp.where(part >= 3, roll(left, 3), 0.0).astype(BF)
    own_l = jnp.where(part >= 5, roll(left, 5), 0.0).astype(BF)
    msg_r = jnp.where(part < 5, roll(right, -3), 0.0).astype(BF)
    own_r = jnp.where(part < 3, roll(right, -5), 0.0).astype(BF)
    return msg_l, msg_r, own_l, own_r


def pack_kernel(image, own, near_row, far_row, far_small, msgs, olds, lo, hi):
    _, inline, depth, _ = image.shape
    odd = lax.axis_index("gx") % 2
    for x in range(inline):

        def store(z, a, b):
            own[z, x, :, :128] = a
            own[z, x, :, 128:] = b

        msg_l, msg_r, own_l, own_r = relayout(image[:, x], lo, hi, store)
        msgs[x, :, :128] = msg_l
        msgs[x, :, 128:] = msg_r
        olds[x, :, :128] = own_l
        olds[x, :, 128:] = own_r
    near, far = (inline - 1) * (1 - odd), (inline - 1) * odd
    near_row[pl.ds(0, depth)] = own[:, near]
    near_row[depth] = msgs[near]
    near_row[depth + 1] = olds[near]
    far_row[...] = own[:, far]
    far_small[0] = msgs[far]
    far_small[1] = olds[far]


def at_map_end():
    at = lax.axis_index("gx")
    return (at == 0) | (at == lax.axis_size("gx") - 1)


def strip_kernel(far_row, mate, msgs, olds, send_1, send_2, strips):
    inline = msgs.shape[0]
    depth = mate.shape[0] - 2
    odd = lax.axis_index("gx") % 2
    outside = at_map_end()
    far, near = (inline + 1) * odd, (inline + 1) * (1 - odd)
    zero = jnp.zeros(strips.shape[1:], BF)
    far_msg = jnp.where(outside, zero, far_row[0])
    near_msg = mate[depth]
    strips[pl.ds(1, inline)] = olds[...]
    strips[near] = mate[depth + 1]
    strips[far] = jnp.where(outside, zero, far_row[1])
    for send, right in ((send_1, odd == 0), (send_2, odd == 1)):

        def pick(v):
            return jnp.where(right, v[..., 128:], v[..., :128])

        send[pl.ds(1, inline)] = pick(msgs[...])
        send[near] = pick(near_msg)
        send[far] = pick(far_msg)


def taps(g, rows):
    return roll(g[:rows], 1) + g[rows : 2 * rows] + roll(g[2 * rows :], -1)


def finish(z, m, bias, acc):
    m = jnp.maximum(jnp.maximum(m, roll(m, -1)) + bias[...], 0.0)
    rows = m.shape[0]
    acc[pl.ds(z * rows, rows), :] = m.astype(BF)


def fill(own, halo, halo_first, pad):
    depth, inline, chans, cross = own.shape
    width = inline * chans
    zero = jnp.zeros((width, cross), BF)
    pad[pl.ds(0, width), :] = zero
    pad[pl.ds((depth + 1) * width, width), :] = zero
    first = 1 - halo_first
    for z in range(depth):
        base = (z + 1) * width
        beyond = zero[:chans] if halo is None else halo[z]
        pad[pl.ds(pl.multiple_of(base + (1 - halo_first) * (inline - 1) * chans, chans), chans), :] = beyond
        for r in range(inline - 1):
            pad[pl.ds(pl.multiple_of(base + (r + halo_first) * chans, chans), chans), :] = own[z, first + r]


def layer_rows(z, a1, pad, width):
    g = dot(a1[...], pad[pl.ds(z * width, 3 * width), :])
    rows = g.shape[0] // 6
    return [taps(g[xo * 3 * rows : (xo + 1) * 3 * rows], rows) for xo in range(2)]


def early_kernel(own, mate, a1, bias, evens, pooled, sums, pad, rest, acc):
    depth, inline, chans, _ = own.shape
    width = inline * chans
    odd = lax.axis_index("gx") % 2
    fill(own, mate, odd, pad)
    fill(own, None, 1 - odd, rest)

    def layer(z):
        rows = layer_rows(z, a1, pad, width)
        return jnp.maximum(rows[0], rows[1])

    for z in range(depth // 2):
        finish(z, jnp.maximum(layer(2 * z), layer(2 * z + 1)), bias, acc)
    pooled[...] = dot(acc[...], evens[...]).astype(BF).reshape(pooled.shape)
    for z in range(depth):
        rows = layer_rows(z, a1, rest, width)
        sums[z, 0] = rows[0]
        sums[z, 1] = rows[1]


def late_kernel(
    sums, halo, early, strips, got_1, got_2, a1h, a1s, bias, evens, message, far_message, pad, acc, edges, rows
):
    depth, _, chans, cross = sums.shape
    half_depth = depth // 2
    odd = lax.axis_index("gx") % 2
    outside = at_map_end()
    edge_columns(strips, got_1, got_2, a1s, bias, edges, rows)
    zero = jnp.zeros((chans, cross), BF)
    pad[pl.ds(0, chans), :] = zero
    pad[pl.ds((depth + 1) * chans, chans), :] = zero
    for z in range(depth):
        pad[pl.ds((z + 1) * chans, chans), :] = jnp.where(outside, zero, halo[z])

    def layer(z):
        g = dot(a1h[odd], pad[pl.ds(z * chans, 3 * chans), :])
        return jnp.maximum(sums[z, odd] + taps(g, chans), sums[z, 1 - odd])

    for z in range(half_depth):
        finish(z, jnp.maximum(layer(2 * z), layer(2 * z + 1)), bias, acc)
    late = dot(acc[...], evens[...]).astype(BF).reshape(early.shape)
    message[odd, pl.ds(0, half_depth)] = late
    message[1 - odd, pl.ds(0, half_depth)] = early[...]
    message[0, half_depth] = edges[0]
    message[1, half_depth] = edges[1]
    far_message[pl.ds(0, half_depth)] = late
    far_message[half_depth] = edges[0]
    far_message[half_depth + 1] = edges[1]


def edge_columns(strips, got_1, got_2, a1s, bias, edges, rows):
    tall, chans, _ = strips.shape
    odd = lax.axis_index("gx") % 2
    at, end = lax.axis_index("gy"), lax.axis_size("gy") - 1
    part = lanes((tall * chans, 128)) % G
    one, two = got_1[...].reshape(tall * chans, 128), got_2[...].reshape(tall * chans, 128)
    from_l = jnp.where(at == 0, 0.0, jnp.where(odd == 0, one, two))
    from_r = jnp.where(at == end, 0.0, jnp.where(odd == 0, two, one))
    s = strips[...].reshape(tall * chans, 256)
    rows[:, :128] = jnp.where(part < 5, from_l, s[:, :128]).astype(BF)
    rows[:, 128:] = jnp.where(part < 3, s[:, 128:], from_r).astype(BF)
    lane = lanes((chans, 128))
    for pair in range(2):
        g = dot(a1s[...], rows[pl.ds(pair * 2 * chans, 4 * chans), :])
        sides = []
        for side in range(2):
            best = None
            for xo in range(2):
                total = None
                for e in range(3):
                    part = None
                    for f in range(3):
                        k = (xo * 3 + e) * 3 + f
                        t = g[k * chans : (k + 1) * chans, side * 128 : side * 128 + 128]
                        t = roll(t, -(G * (e - 1) + f - 1))
                        part = t if part is None else part + t
                    if e == 0:
                        part = jnp.where(lane >= G, part, 0.0)
                    if e == 2:
                        part = jnp.where(lane < 128 - G, part, 0.0)
                    total = part if total is None else total + part
                best = total if best is None else jnp.maximum(best, total)
            best = jnp.maximum(best, roll(best, -G))
            best = jnp.maximum(best, roll(best, -1))
            best = jnp.maximum(best + bias[:, :128], 0.0)
            cell = lane % G
            outside = (cell < 5) & (at == 0) if side == 0 else (cell > 1) & (at == end)
            sides.append(jnp.where(outside, 0.0, best))
        edges[pair] = jnp.where((lane // G) % 2 == 0, sides[0], roll(sides[1], G)).astype(BF)


def assemble(cells, columns, depth, ends, outside, pad, edge):
    coarse = 2
    width, half = edge.shape
    chans = width // coarse
    zero = jnp.zeros((width, 256), BF)
    pad[pl.ds(0, width), :] = zero
    pad[pl.ds((depth + 1) * width, width), :] = zero

    def hide(v):
        return v if outside is None else jnp.where(outside, zero[:chans, :half], v)

    for r in range(coarse):
        edge[pl.ds(r * chans, chans), :] = hide(columns(r))
    lane = lanes((chans, half))
    inner = (lane > 0) & (lane < half - 1)
    for z in range(depth):
        fixed = dot(edge[...], ends[pl.ds(half - 2 * G - 2 * G * z, half), :]).astype(BF)
        base = (z + 1) * width
        pad[pl.ds(base, width), half:] = fixed[:, half:]
        for r in range(coarse):
            spot = pl.ds(base + r * chans, chans)
            pad[spot, :half] = jnp.where(inner, hide(cells(r, z)), fixed[r * chans : (r + 1) * chans, :half])


def keep(q, z, r, v):
    rows = v.shape[0]
    half = v.shape[1] // 2
    for f in range(3):
        s = v if f == 1 else roll(v, 1 - f)
        s = s[:, :half].astype(BF)
        q[pl.ds(((z * 3 + f) * 2 + r) * rows, rows), half:] = s
        q[pl.ds((((z + 1) * 3 + f) * 2 + r) * rows, rows), :half] = s


def clear(q, depth):
    rows = q.shape[0] // (depth + 1)
    half = q.shape[1] // 2
    q[pl.ds(0, rows), :half] = jnp.zeros((rows, half), BF)
    q[pl.ds(depth * rows, rows), half:] = jnp.zeros((rows, half), BF)


def beyond_cross(c2, half):
    at, end = lax.axis_index("gy"), lax.axis_size("gy") - 1
    col = lanes((c2, 2 * half))
    return ((col == 2 * half - 1) & (at == 0)) | ((col == half) & (at == end))


def coarse_own_kernel(own, a2, ends, near, part2, pad, edge):
    coarse, tall, chans, _ = own.shape
    depth = tall - 1
    odd = lax.axis_index("gx") % 2
    width = coarse * chans
    c2 = near.shape[2]
    assemble(lambda r, z: own[r, z], lambda r: own[r, depth], depth, ends, None, pad, edge)
    for z in range(depth):
        window = pl.ds(z * width, 3 * width)
        for half_of, into in ((odd, near), (1 - odd, part2)):
            g = dot(a2[half_of], pad[window, :])
            for xo in range(2):
                into[z, xo] = taps(g[xo * 3 * c2 : (xo + 1) * 3 * c2], c2)


def coarse_near_kernel(mate, near, a2, b2, a3, ends, part3, pad, edge, q):
    coarse, tall, chans, half = mate.shape
    depth = tall - 1
    c2 = b2.shape[0]
    odd = lax.axis_index("gx") % 2
    width = coarse * chans
    assemble(lambda r, z: mate[r, z], lambda r: mate[r, depth], depth, ends, None, pad, edge)
    clear(q, depth)
    hide = beyond_cross(c2, half)
    for z in range(depth):
        g = dot(a2[1 - odd], pad[pl.ds(z * width, 3 * width), :])
        for xo in range(2):
            v = taps(g[xo * 3 * c2 : (xo + 1) * 3 * c2], c2) + near[z, xo]
            v = jnp.maximum(v + b2[...], 0.0)
            keep(q, z, xo, jnp.where(hide, 0.0, v))
    rows = 6 * c2
    for z in range(0, depth, 2):
        part3[z // 2] = dot(a3[1 - odd], q[pl.ds(z * rows, 3 * rows), :])


def coarse_far_kernel(first, far, part2, part3, a2, b2, a3, b3, ends, out, pad, edge, q, wide):
    depth, chans, half = first.shape
    coarse = out.shape[1]
    c2 = b2.shape[0]
    odd = lax.axis_index("gx") % 2
    at, end = lax.axis_index("gx"), lax.axis_size("gx") - 1
    width = coarse * chans

    def cells(r, z):
        return jnp.where(odd == r, first[z], far[z])

    assemble(cells, lambda r: far[depth + r], depth, ends, at_map_end(), pad, edge)
    clear(q, depth)
    outside = [(odd == 0) & (at == 0), (odd == 1) & (at == end)]
    hide = beyond_cross(c2, half)
    for z in range(depth):
        g = dot(a2[odd], pad[pl.ds(z * width, 3 * width), :])
        for xo in range(2):
            v = taps(g[xo * 3 * c2 : (xo + 1) * 3 * c2], c2) + part2[z, xo]
            v = jnp.maximum(v + b2[...], 0.0)
            keep(q, z, xo, jnp.where(hide | outside[xo], 0.0, v))
    rows = 6 * c2
    for z in range(0, depth, 2):
        g = dot(a3[odd], q[pl.ds(z * rows, 3 * rows), :]) + part3[z // 2]
        for xo in range(2):
            v = jnp.maximum(g[xo * c2 : (xo + 1) * c2] + b3[...], 0.0)
            wide[xo, pl.ds(z, c2, stride=depth), :] = v[:, :half]
            wide[xo, pl.ds(z + 1, c2, stride=depth), :] = v[:, half:]
    for xo in range(coarse):
        out[:, xo] = wide[xo].reshape(c2, depth, half).astype(BF)


def permute(value, target):
    wide, deep = lax.axis_size("gx"), lax.axis_size("gy")
    pairs = []
    for x in range(wide):
        for y in range(deep):
            tx, ty = target(x, y, wide, deep)
            pairs.append((x * deep + y, tx * deep + ty))
    return lax.ppermute(value, ("gx", "gy"), pairs)


def mate_of(x, y, wide, deep):
    return x ^ 1, y


def far_of(x, y, wide, deep):
    to = x + 1 if x % 2 else x - 1
    if 0 <= to < wide:
        return to, y
    if deep % 2 == 0:
        return x, y ^ 1
    return to % wide, y


def loop_of(up):
    def target(x, y, wide, deep):
        to = y + 1 if (x % 2 == 0) == up else y - 1
        return (x, to) if 0 <= to < deep else (x ^ 1, y)

    return target


def per_device(image, w_first, b_first, w_second, b_second, w_third, b_third):
    c1, inline, depth, cross = image.shape
    c2 = w_third.shape[0]
    half, hz, coarse = cross // 2, depth // 2, inline // 2
    k1 = 4 * c1
    tall = inline + 2
    own, near_row, far_row, far_small, msgs, olds = call(
        pack_kernel,
        [
            ((depth, inline, c1, cross), BF),
            ((depth + 2, c1, cross), BF),
            ((depth, c1, cross), BF),
            ((2, c1, 256), BF),
            ((inline, c1, 256), BF),
            ((inline, c1, 256), BF),
        ],
        scratch=[pltpu.VMEM((c1 * depth, 128), F32)] * 2,
        flops=1 << 28,
    )(image)
    got_small = permute(far_small, far_of)
    got_far = permute(far_row, far_of)
    got_row = permute(near_row, mate_of)
    a1, a1s, a1h, a2, a3, b1, b2, b3, evens, ends = call(
        weights_kernel,
        [
            ((6 * c1, 3 * k1), BF),
            ((18 * c1, k1), BF),
            ((2, 3 * c1, 3 * c1), BF),
            ((2, 6 * c2, 6 * c1), BF),
            ((2, 2 * c2, 18 * c2), BF),
            ((c1, 256), F32),
            ((c2, 256), F32),
            ((c2, 256), F32),
            ((cross, half), BF),
            ((2 * half, 256), BF),
        ],
        flops=1 << 28,
    )(
        jnp.transpose(w_first, (2, 3, 4, 0, 1)),
        jnp.transpose(w_second, (2, 3, 4, 1, 0)),
        jnp.transpose(w_third, (2, 3, 4, 0, 1)),
        b_first.reshape(1, c1),
        b_second.reshape(1, c2),
        b_third.reshape(1, c2),
    )
    fine = [pltpu.VMEM(((depth + 2) * k1, cross), BF), pltpu.VMEM((hz * c1, cross), BF)]
    early, sums = call(
        early_kernel, [((hz, c1, half), BF), ((depth, 2, c1, cross), F32)], scratch=fine[:1] + fine, flops=1 << 30
    )(own, got_row, a1, b1, evens)
    send_1, send_2, strips = call(
        strip_kernel, [((tall, c1, 128), BF)] * 2 + [((tall, c1, 256), BF)], flops=1 << 20
    )(got_small, got_row, msgs, olds)
    got_1 = permute(send_1, loop_of(True))
    got_2 = permute(send_2, loop_of(False))
    got_first = permute(early, far_of)
    message, far_message = call(
        late_kernel,
        [((coarse, hz + 1, c1, half), BF), ((hz + 2, c1, half), BF)],
        scratch=[
            pltpu.VMEM(((depth + 2) * c1, cross), BF),
            pltpu.VMEM((hz * c1, cross), BF),
            pltpu.VMEM((coarse, c1, half), BF),
            pltpu.VMEM((tall * c1, 256), BF),
        ],
        flops=1 << 28,
    )(sums, got_far, early, strips, got_1, got_2, a1h, a1s, b1, evens)
    got_pa = permute(message, mate_of)
    got_pb = permute(far_message, far_of)
    pad = pltpu.VMEM(((hz + 2) * 2 * c1, 256), BF)
    edge = pltpu.VMEM((2 * c1, half), BF)
    q = pltpu.VMEM(((hz + 1) * 6 * c2, 256), BF)
    near, part2 = call(
        coarse_own_kernel, [((hz, 2, c2, 256), F32)] * 2, scratch=[pad, edge], flops=1 << 29
    )(message, a2, ends)
    (part3,) = call(
        coarse_near_kernel, [((hz // 2, 2 * c2, 256), F32)], scratch=[pad, edge, q], flops=1 << 29
    )(got_pa, near, a2, b2, a3, ends)
    (out,) = call(
        coarse_far_kernel,
        [((c2, coarse, hz, half), BF)],
        scratch=[pad, edge, q, pltpu.VMEM((coarse, c2 * hz, half), F32)],
        flops=1 << 29,
    )(got_first, got_pb, part2, part3, a2, b2, a3, b3, ends)
    return out


def solution(mesh):
    placed = (P(None, "gx", None, "gy"), P(), P(), P(), P(), P(), P())

    return jax.shard_map(per_device, mesh=mesh, in_specs=placed, out_specs=P(None, "gx", None, "gy"), check_vma=False)
```

```python
import jax
import jax.numpy as jnp
from jax import lax
from jax.experimental import pallas as pl
from jax.experimental.pallas import tpu as pltpu
from jax.sharding import PartitionSpec as P


BF = jnp.bfloat16
F32 = jnp.float32
VM = pl.BlockSpec(memory_space=pltpu.VMEM)
G = 8


def call(body, outs, scratch=(), flops=0, space=pltpu.VMEM, limit=16):
    def run(*args):
        return pl.pallas_call(
            body,
            out_shape=[jax.ShapeDtypeStruct(s, d) for s, d in outs],
            in_specs=[pl.BlockSpec(memory_space=space)] * len(args),
            out_specs=[VM] * len(outs),
            scratch_shapes=list(scratch),
            compiler_params=pltpu.CompilerParams(vmem_limit_bytes=limit << 20),
            cost_estimate=pl.CostEstimate(flops=flops, bytes_accessed=1 << 20, transcendentals=0),
        )(*args)

    return run


def dot(a, b):
    return jnp.dot(a, b, preferred_element_type=F32)


def lanes(shape):
    return lax.broadcasted_iota(jnp.int32, shape, len(shape) - 1)


def roll(v, by):
    return pltpu.roll(v, by % v.shape[-1], v.ndim - 1)


def weights_kernel(w1, w2, w3, b1, b2, b3, a1, a1s, a1h, a2, a3, c1, c2, c3, evens, ends):
    n1, n2 = w1.shape[3], w3.shape[3]
    zero1, zero3 = jnp.zeros((n1, n1), F32), jnp.zeros((n2, n2), F32)
    zero2 = jnp.zeros((n2, n1), F32)
    p1, p2, p3 = {}, {}, {}
    for e in range(3):
        for f in range(3):
            for a in range(-1, 4):
                inside = 0 <= a < 3
                p1[a, e, f] = w1[a, e, f].astype(F32) if inside else zero1
                p2[a, e, f] = w2[a, e, f].astype(F32).T if inside else zero2
                p3[a, e, f] = w3[a, e, f].astype(F32) if inside else zero3
    join = lambda pieces: jnp.concatenate(pieces, axis=1).astype(BF)
    for xo in range(2):
        for f in range(3):
            for e in range(3):
                v = join([p1[xi - xo, e, f] for xi in range(4)])
                a1[pl.ds((xo * 3 + f) * n1, n1), pl.ds(e * 4 * n1, 4 * n1)] = v
                a1s[pl.ds(((xo * 3 + e) * 3 + f) * n1, n1), :] = v
            for h in range(2):
                for e in range(3):
                    spot = pl.ds((e * 3 + f) * 2 * n2, 2 * n2)
                    a3[h, pl.ds(xo * n2, n2), spot] = join([p3[2 * h + r - xo, e, f] for r in range(2)])
    for h in range(2):
        for xo in range(2):
            row = [p2[2 * h + r - xo, e, f] for e in range(3) for f in range(3) for r in range(2)]
            a2[h, pl.ds(xo * n2, n2), :] = join(row)
        for f in range(3):
            a1h[h, pl.ds(f * n1, n1), :] = join([p1[2 * h, e, f] for e in range(3)])
    for b, c in ((b1, c1), (b2, c2), (b3, c3)):
        n = b.shape[1]
        eye = lax.broadcasted_iota(jnp.int32, (n, n), 0) == lax.broadcasted_iota(jnp.int32, (n, n), 1)
        column = jnp.sum(jnp.where(eye, jnp.broadcast_to(b[...], (n, n)), 0.0), axis=1, keepdims=True)
        c[...] = jnp.broadcast_to(column, c.shape)
    src = lax.broadcasted_iota(jnp.int32, evens.shape, 0)
    dst = lax.broadcasted_iota(jnp.int32, evens.shape, 1)
    evens[...] = jnp.where(src == 2 * dst, 1.0, 0.0).astype(BF)
    half = evens.shape[1]
    top = half - 2 * G
    src = lax.broadcasted_iota(jnp.int32, ends.shape, 0) - top
    dst = lax.broadcasted_iota(jnp.int32, ends.shape, 1)
    move = (
        ((dst == 0) & (src == 5))
        | ((dst == half - 1) & (src == G + 1))
        | ((dst == half) & (src == G + 3))
        | ((dst == half + 1) & (src == G + 5))
        | ((dst == 254) & (src == 1))
        | ((dst == 255) & (src == 3))
    )
    ends[...] = jnp.where(move, 1.0, 0.0).astype(BF)


def relayout(cells, lo, hi, store):
    chans, depth, cross = cells.shape
    flat = cells.astype(F32).reshape(chans * depth, cross)
    lo[...] = flat[:, :128]
    hi[...] = flat[:, 128:]
    lane = lanes((chans, 128))
    left = jnp.zeros((chans, 128), F32)
    right = jnp.zeros((chans, 128), F32)
    for z in range(depth):
        a = lo[pl.ds(z, chans, stride=depth), :]
        b = hi[pl.ds(z, chans, stride=depth), :]
        store(z, a.astype(BF), b.astype(BF))
        here = (lane >= z * G) & (lane < z * G + G)
        left = jnp.where(here, roll(a, z * G), left)
        right = jnp.where(here, roll(b, z * G + G), right)
    part = lane % G
    msg_l = jnp.where(part >= 3, roll(left, 3), 0.0).astype(BF)
    own_l = jnp.where(part >= 5, roll(left, 5), 0.0).astype(BF)
    msg_r = jnp.where(part < 5, roll(right, -3), 0.0).astype(BF)
    own_r = jnp.where(part < 3, roll(right, -5), 0.0).astype(BF)
    return msg_l, msg_r, own_l, own_r


def row_kernel(image, local, far_row, far_small, lo, hi, sems):
    inline = image.shape[1]
    far = (inline - 1) * (lax.axis_index("gx") % 2)
    copies = []
    for k in range(inline):
        x = (far + k) % inline
        copies.append(pltpu.make_async_copy(image.at[:, x], local.at[x], sems.at[k]))
        copies[k].start()
    copies[0].wait()

    def store(z, a, b):
        far_row[z, :, :128] = a
        far_row[z, :, 128:] = b

    msg_l, msg_r, own_l, own_r = relayout(local[far], lo, hi, store)
    far_small[0, :, :128] = msg_l
    far_small[0, :, 128:] = msg_r
    far_small[1, :, :128] = own_l
    far_small[1, :, 128:] = own_r
    for copy in copies[1:]:
        copy.wait()


def pack_kernel(local, far_row, far_small, own, near_row, msgs, olds, lo, hi):
    inline, _, depth, _ = local.shape
    odd = lax.axis_index("gx") % 2
    near, far = (inline - 1) * (1 - odd), (inline - 1) * odd
    own[:, far] = far_row[...]
    msgs[far] = far_small[0]
    olds[far] = far_small[1]
    for k in range(1, inline):
        x = (far + k) % inline

        def store(z, a, b):
            own[z, x, :, :128] = a
            own[z, x, :, 128:] = b

        msg_l, msg_r, own_l, own_r = relayout(local[x], lo.at[k - 1], hi.at[k - 1], store)
        msgs[x, :, :128] = msg_l
        msgs[x, :, 128:] = msg_r
        olds[x, :, :128] = own_l
        olds[x, :, 128:] = own_r
    near_row[pl.ds(0, depth)] = own[:, near]
    near_row[depth] = msgs[near]
    near_row[depth + 1] = olds[near]


def at_map_end():
    at = lax.axis_index("gx")
    return (at == 0) | (at == lax.axis_size("gx") - 1)


def strip_kernel(far_row, mate, msgs, olds, send_1, send_2, strips):
    inline = msgs.shape[0]
    depth = mate.shape[0] - 2
    odd = lax.axis_index("gx") % 2
    outside = at_map_end()
    far, near = (inline + 1) * odd, (inline + 1) * (1 - odd)
    zero = jnp.zeros(strips.shape[1:], BF)
    far_msg = jnp.where(outside, zero, far_row[0])
    near_msg = mate[depth]
    strips[pl.ds(1, inline)] = olds[...]
    strips[near] = mate[depth + 1]
    strips[far] = jnp.where(outside, zero, far_row[1])
    for send, right in ((send_1, odd == 0), (send_2, odd == 1)):

        def pick(v):
            return jnp.where(right, v[..., 128:], v[..., :128])

        send[pl.ds(1, inline)] = pick(msgs[...])
        send[near] = pick(near_msg)
        send[far] = pick(far_msg)


def taps(g, rows):
    return roll(g[:rows], 1) + g[rows : 2 * rows] + roll(g[2 * rows :], -1)


def finish(z, m, bias, acc):
    m = jnp.maximum(jnp.maximum(m, roll(m, -1)) + bias[...], 0.0)
    rows = m.shape[0]
    acc[pl.ds(z * rows, rows), :] = m.astype(BF)


def fill(own, halo, halo_first, pad):
    depth, inline, chans, cross = own.shape
    width = inline * chans
    zero = jnp.zeros((width, cross), BF)
    pad[pl.ds(0, width), :] = zero
    pad[pl.ds((depth + 1) * width, width), :] = zero
    first = 1 - halo_first
    for z in range(depth):
        base = (z + 1) * width
        beyond = zero[:chans] if halo is None else halo[z]
        pad[pl.ds(pl.multiple_of(base + (1 - halo_first) * (inline - 1) * chans, chans), chans), :] = beyond
        for r in range(inline - 1):
            pad[pl.ds(pl.multiple_of(base + (r + halo_first) * chans, chans), chans), :] = own[z, first + r]


def layer_rows(z, a1, pad, width):
    g = dot(a1[...], pad[pl.ds(z * width, 3 * width), :])
    rows = g.shape[0] // 6
    return [taps(g[xo * 3 * rows : (xo + 1) * 3 * rows], rows) for xo in range(2)]


def early_kernel(own, mate, a1, bias, evens, pooled, sums, pad, rest, acc):
    depth, inline, chans, _ = own.shape
    width = inline * chans
    odd = lax.axis_index("gx") % 2
    fill(own, mate, odd, pad)
    fill(own, None, 1 - odd, rest)

    def layer(z):
        rows = layer_rows(z, a1, pad, width)
        return jnp.maximum(rows[0], rows[1])

    for z in range(depth // 2):
        finish(z, jnp.maximum(layer(2 * z), layer(2 * z + 1)), bias, acc)
    pooled[...] = dot(acc[...], evens[...]).astype(BF).reshape(pooled.shape)
    for z in range(depth):
        rows = layer_rows(z, a1, rest, width)
        sums[z, 0] = rows[0]
        sums[z, 1] = rows[1]


def late_kernel(
    sums, halo, early, strips, got_1, got_2, a1h, a1s, bias, evens, message, far_message, pad, acc, edges, rows
):
    depth, _, chans, cross = sums.shape
    half_depth = depth // 2
    odd = lax.axis_index("gx") % 2
    outside = at_map_end()
    edge_columns(strips, got_1, got_2, a1s, bias, edges, rows)
    zero = jnp.zeros((chans, cross), BF)
    pad[pl.ds(0, chans), :] = zero
    pad[pl.ds((depth + 1) * chans, chans), :] = zero
    for z in range(depth):
        pad[pl.ds((z + 1) * chans, chans), :] = jnp.where(outside, zero, halo[z])

    def layer(z):
        g = dot(a1h[odd], pad[pl.ds(z * chans, 3 * chans), :])
        return jnp.maximum(sums[z, odd] + taps(g, chans), sums[z, 1 - odd])

    for z in range(half_depth):
        finish(z, jnp.maximum(layer(2 * z), layer(2 * z + 1)), bias, acc)
    late = dot(acc[...], evens[...]).astype(BF).reshape(early.shape)
    message[odd, pl.ds(0, half_depth)] = late
    message[1 - odd, pl.ds(0, half_depth)] = early[...]
    message[0, half_depth] = edges[0]
    message[1, half_depth] = edges[1]
    far_message[pl.ds(0, half_depth)] = late
    far_message[half_depth] = edges[0]
    far_message[half_depth + 1] = edges[1]


def edge_columns(strips, got_1, got_2, a1s, bias, edges, rows):
    tall, chans, _ = strips.shape
    odd = lax.axis_index("gx") % 2
    at, end = lax.axis_index("gy"), lax.axis_size("gy") - 1
    part = lanes((tall * chans, 128)) % G
    one, two = got_1[...].reshape(tall * chans, 128), got_2[...].reshape(tall * chans, 128)
    from_l = jnp.where(at == 0, 0.0, jnp.where(odd == 0, one, two))
    from_r = jnp.where(at == end, 0.0, jnp.where(odd == 0, two, one))
    s = strips[...].reshape(tall * chans, 256)
    rows[:, :128] = jnp.where(part < 5, from_l, s[:, :128]).astype(BF)
    rows[:, 128:] = jnp.where(part < 3, s[:, 128:], from_r).astype(BF)
    lane = lanes((chans, 128))
    for pair in range(2):
        g = dot(a1s[...], rows[pl.ds(pair * 2 * chans, 4 * chans), :])
        sides = []
        for side in range(2):
            best = None
            for xo in range(2):
                total = None
                for e in range(3):
                    part = None
                    for f in range(3):
                        k = (xo * 3 + e) * 3 + f
                        t = g[k * chans : (k + 1) * chans, side * 128 : side * 128 + 128]
                        t = roll(t, -(G * (e - 1) + f - 1))
                        part = t if part is None else part + t
                    if e == 0:
                        part = jnp.where(lane >= G, part, 0.0)
                    if e == 2:
                        part = jnp.where(lane < 128 - G, part, 0.0)
                    total = part if total is None else total + part
                best = total if best is None else jnp.maximum(best, total)
            best = jnp.maximum(best, roll(best, -G))
            best = jnp.maximum(best, roll(best, -1))
            best = jnp.maximum(best + bias[:, :128], 0.0)
            cell = lane % G
            outside = (cell < 5) & (at == 0) if side == 0 else (cell > 1) & (at == end)
            sides.append(jnp.where(outside, 0.0, best))
        edges[pair] = jnp.where((lane // G) % 2 == 0, sides[0], roll(sides[1], G)).astype(BF)


def assemble(cells, columns, depth, ends, outside, q2, eb):
    coarse = 2
    half = eb.shape[1]
    chans = q2.shape[0] // (depth + 1) // 6
    width = coarse * chans
    zero = jnp.zeros((chans, half), BF)

    def hide(v):
        return v if outside is None else jnp.where(outside, zero, v)

    edge = jnp.concatenate([hide(columns(r)) for r in range(coarse)], axis=0)
    flat = edge.astype(F32)
    lane = lanes((width, half))
    for e in range(3):
        for f in range(3):
            by = 2 * G * (e - 1) + 2 * (f - 1)
            v = roll(flat, -by) if by else flat
            if e == 0:
                v = jnp.where(lane >= 2 * G, v, 0.0)
            if e == 2:
                v = jnp.where(lane < half - 2 * G, v, 0.0)
            eb[pl.ds((e * 3 + f) * width, width), :] = v.astype(BF)
    clear(q2, depth)
    lane = lanes((chans, half))
    inner = (lane > 0) & (lane < half - 1)
    for z in range(depth):
        fixed = dot(edge, ends[pl.ds(half - 2 * G - 2 * G * z, half), :])
        for r in range(coarse):
            own = fixed[r * chans : (r + 1) * chans]
            main = jnp.where(inner, hide(cells(r, z)).astype(F32), own[:, :half])
            keep(q2, z, r, jnp.concatenate([main, own[:, half:]], axis=1))


def keep(q, z, r, v):
    rows = v.shape[0]
    half = v.shape[1] // 2
    for f in range(3):
        s = v if f == 1 else roll(v, 1 - f)
        s = s[:, :half].astype(BF)
        q[pl.ds(((z * 3 + f) * 2 + r) * rows, rows), half:] = s
        q[pl.ds((((z + 1) * 3 + f) * 2 + r) * rows, rows), :half] = s


def clear(q, depth):
    rows = q.shape[0] // (depth + 1)
    half = q.shape[1] // 2
    q[pl.ds(0, rows), :half] = jnp.zeros((rows, half), BF)
    q[pl.ds(depth * rows, rows), half:] = jnp.zeros((rows, half), BF)


def coarse_own_kernel(own, a2, ends, near, near_ends, part2, part2_ends, q2, eb):
    _, tall, chans, _ = own.shape
    depth = tall - 1
    odd = lax.axis_index("gx") % 2
    assemble(lambda r, z: own[r, z], lambda r: own[r, depth], depth, ends, None, q2, eb)
    rows = 6 * chans
    for part, into, into_ends in ((odd, near, near_ends), (1 - odd, part2, part2_ends)):
        for z in range(0, depth, 2):
            into[z // 2] = dot(a2[part], q2[pl.ds(z * rows, 3 * rows), :])
        into_ends[...] = dot(a2[part], eb[...])


def first_map(part, a2, b2, add, add_ends, outside, q2, eb, q, depth):
    half = eb.shape[1]
    c2 = b2.shape[0]
    at, end = lax.axis_index("gy"), lax.axis_size("gy") - 1
    rows = q2.shape[0] // (depth + 1)
    lane = lanes((c2, half))
    left = (lane % (2 * G)) < G
    beyond = (left & (at == 0)) | (~left & (at == end))
    clear(q, depth)
    g = dot(a2[part], eb[...]) + add_ends[...]
    ends = []
    for xo in range(2):
        v = jnp.maximum(g[xo * c2 : (xo + 1) * c2] + b2[:, :half], 0.0)
        ends.append(jnp.where(beyond, 0.0, v))
    for z in range(0, depth, 2):
        g = dot(a2[part], q2[pl.ds(z * rows, 3 * rows), :]) + add[z // 2]
        for xo in range(2):
            v = jnp.maximum(g[xo * c2 : (xo + 1) * c2] + b2[...], 0.0)
            for k in range(2):
                spot = 2 * G * (z + k) + 3
                right = roll(ends[xo], -(spot + G))
                before = roll(ends[xo], half - 1 - spot)
                side = jnp.where(lane == 0, right, before)
                w = jnp.concatenate([v[:, k * half : (k + 1) * half], side], axis=1)
                if outside is not None:
                    w = jnp.where(outside[xo], 0.0, w)
                keep(q, z + k, xo, w)


def coarse_near_kernel(mate, near, near_ends, a2, b2, a3, ends, part3, q2, eb, q):
    _, tall, _, _ = mate.shape
    depth = tall - 1
    c2 = b2.shape[0]
    odd = lax.axis_index("gx") % 2
    assemble(lambda r, z: mate[r, z], lambda r: mate[r, depth], depth, ends, None, q2, eb)
    first_map(1 - odd, a2, b2, near, near_ends, None, q2, eb, q, depth)
    rows = 6 * c2
    for z in range(0, depth, 2):
        part3[z // 2] = dot(a3[1 - odd], q[pl.ds(z * rows, 3 * rows), :])


def coarse_far_kernel(first, far, part2, part2_ends, part3, a2, b2, a3, b3, ends, out, q2, eb, q, wide):
    depth, _, half = first.shape
    coarse = out.shape[1]
    c2 = b2.shape[0]
    odd = lax.axis_index("gx") % 2
    at, end = lax.axis_index("gx"), lax.axis_size("gx") - 1

    def cells(r, z):
        return jnp.where(odd == r, first[z], far[z])

    assemble(cells, lambda r: far[depth + r], depth, ends, at_map_end(), q2, eb)
    outside = [(odd == 0) & (at == 0), (odd == 1) & (at == end)]
    first_map(odd, a2, b2, part2, part2_ends, outside, q2, eb, q, depth)
    rows = 6 * c2
    for z in range(0, depth, 2):
        g = dot(a3[odd], q[pl.ds(z * rows, 3 * rows), :]) + part3[z // 2]
        for xo in range(2):
            v = jnp.maximum(g[xo * c2 : (xo + 1) * c2] + b3[...], 0.0)
            wide[xo, pl.ds(z, c2, stride=depth), :] = v[:, :half]
            wide[xo, pl.ds(z + 1, c2, stride=depth), :] = v[:, half:]
    for xo in range(coarse):
        out[:, xo] = wide[xo].reshape(c2, depth, half).astype(BF)


def permute(value, target):
    wide, deep = lax.axis_size("gx"), lax.axis_size("gy")
    pairs = []
    for x in range(wide):
        for y in range(deep):
            tx, ty = target(x, y, wide, deep)
            pairs.append((x * deep + y, tx * deep + ty))
    return lax.ppermute(value, ("gx", "gy"), pairs)


def mate_of(x, y, wide, deep):
    return x ^ 1, y


def far_of(x, y, wide, deep):
    to = x + 1 if x % 2 else x - 1
    if 0 <= to < wide:
        return to, y
    if deep % 2 == 0:
        return x, y ^ 1
    return to % wide, y


def loop_of(up):
    def target(x, y, wide, deep):
        to = y + 1 if (x % 2 == 0) == up else y - 1
        return (x, to) if 0 <= to < deep else (x ^ 1, y)

    return target


def per_device(image, w_first, b_first, w_second, b_second, w_third, b_third):
    c1, inline, depth, cross = image.shape
    c2 = w_third.shape[0]
    half, hz, coarse = cross // 2, depth // 2, inline // 2
    k1 = 4 * c1
    tall = inline + 2
    local, far_row, far_small = call(
        row_kernel,
        [((inline, c1, depth, cross), BF), ((depth, c1, cross), BF), ((2, c1, 256), BF)],
        scratch=[pltpu.VMEM((c1 * depth, 128), F32)] * 2 + [pltpu.SemaphoreType.DMA((inline,))],
        flops=1 << 20,
        space=pltpu.MemorySpace.HBM,
        limit=52,
    )(image)
    got_small = permute(far_small, far_of)
    got_far = permute(far_row, far_of)
    own, near_row, msgs, olds = call(
        pack_kernel,
        [
            ((depth, inline, c1, cross), BF),
            ((depth + 2, c1, cross), BF),
            ((inline, c1, 256), BF),
            ((inline, c1, 256), BF),
        ],
        scratch=[pltpu.VMEM((inline - 1, c1 * depth, 128), F32)] * 2,
        flops=1 << 28,
    )(local, far_row, far_small)
    got_row = permute(near_row, mate_of)
    a1, a1s, a1h, a2, a3, b1, b2, b3, evens, ends = call(
        weights_kernel,
        [
            ((6 * c1, 3 * k1), BF),
            ((18 * c1, k1), BF),
            ((2, 3 * c1, 3 * c1), BF),
            ((2, 2 * c2, 18 * c1), BF),
            ((2, 2 * c2, 18 * c2), BF),
            ((c1, 256), F32),
            ((c2, 256), F32),
            ((c2, 256), F32),
            ((cross, half), BF),
            ((2 * half, 256), BF),
        ],
        flops=1 << 28,
    )(
        jnp.transpose(w_first, (2, 3, 4, 0, 1)),
        jnp.transpose(w_second, (2, 3, 4, 1, 0)),
        jnp.transpose(w_third, (2, 3, 4, 0, 1)),
        b_first.reshape(1, c1),
        b_second.reshape(1, c2),
        b_third.reshape(1, c2),
    )
    fine = [pltpu.VMEM(((depth + 2) * k1, cross), BF), pltpu.VMEM((hz * c1, cross), BF)]
    early, sums = call(
        early_kernel, [((hz, c1, half), BF), ((depth, 2, c1, cross), F32)], scratch=fine[:1] + fine, flops=1 << 30
    )(own, got_row, a1, b1, evens)
    send_1, send_2, strips = call(
        strip_kernel, [((tall, c1, 128), BF)] * 2 + [((tall, c1, 256), BF)], flops=1 << 20
    )(got_small, got_row, msgs, olds)
    got_1 = permute(send_1, loop_of(True))
    got_2 = permute(send_2, loop_of(False))
    got_first = permute(early, far_of)
    message, far_message = call(
        late_kernel,
        [((coarse, hz + 1, c1, half), BF), ((hz + 2, c1, half), BF)],
        scratch=[
            pltpu.VMEM(((depth + 2) * c1, cross), BF),
            pltpu.VMEM((hz * c1, cross), BF),
            pltpu.VMEM((coarse, c1, half), BF),
            pltpu.VMEM((tall * c1, 256), BF),
        ],
        flops=1 << 28,
    )(sums, got_far, early, strips, got_1, got_2, a1h, a1s, b1, evens)
    got_pa = permute(message, mate_of)
    got_pb = permute(far_message, far_of)
    q2 = pltpu.VMEM(((hz + 1) * 6 * c1, 256), BF)
    eb = pltpu.VMEM((18 * c1, half), BF)
    q = pltpu.VMEM(((hz + 1) * 6 * c2, 256), BF)
    sums2 = [((hz // 2, 2 * c2, 256), F32), ((2 * c2, half), F32)]
    near, near_ends, part2, part2_ends = call(
        coarse_own_kernel, sums2 * 2, scratch=[q2, eb], flops=1 << 29
    )(message, a2, ends)
    (part3,) = call(
        coarse_near_kernel, [((hz // 2, 2 * c2, 256), F32)], scratch=[q2, eb, q], flops=1 << 29
    )(got_pa, near, near_ends, a2, b2, a3, ends)
    (out,) = call(
        coarse_far_kernel,
        [((c2, coarse, hz, half), BF)],
        scratch=[q2, eb, q, pltpu.VMEM((coarse, c2 * hz, half), F32)],
        flops=1 << 29,
    )(got_first, got_pb, part2, part2_ends, part3, a2, b2, a3, b3, ends)
    return out


def solution(mesh):
    placed = (P(None, "gx", None, "gy"), P(), P(), P(), P(), P(), P())

    return jax.shard_map(per_device, mesh=mesh, in_specs=placed, out_specs=P(None, "gx", None, "gy"), check_vma=False)
```

```python
import jax
import jax.numpy as jnp
from jax import lax
from jax.experimental import pallas as pl
from jax.experimental.pallas import tpu as pltpu
from jax.sharding import PartitionSpec as P


BF = jnp.bfloat16
F32 = jnp.float32
VM = pl.BlockSpec(memory_space=pltpu.VMEM)
G = 8


def call(body, outs, scratch=(), flops=0, space=pltpu.VMEM, limit=16):
    def run(*args):
        return pl.pallas_call(
            body,
            out_shape=[jax.ShapeDtypeStruct(s, d) for s, d in outs],
            in_specs=[pl.BlockSpec(memory_space=space)] * len(args),
            out_specs=[VM] * len(outs),
            scratch_shapes=list(scratch),
            compiler_params=pltpu.CompilerParams(vmem_limit_bytes=limit << 20),
            cost_estimate=pl.CostEstimate(flops=flops, bytes_accessed=1 << 20, transcendentals=0),
        )(*args)

    return run


def dot(a, b):
    return jnp.dot(a, b, preferred_element_type=F32)


def lanes(shape):
    return lax.broadcasted_iota(jnp.int32, shape, len(shape) - 1)


def roll(v, by):
    return pltpu.roll(v, by % v.shape[-1], v.ndim - 1)


def weights_kernel(w1, w2, w3, b1, b2, b3, a1, a1s, a1h, a2, a3, c1, c2, c3, evens, ends):
    n1, n2 = w1.shape[3], w3.shape[3]
    zero1, zero3 = jnp.zeros((n1, n1), F32), jnp.zeros((n2, n2), F32)
    zero2 = jnp.zeros((n2, n1), F32)
    p1, p2, p3 = {}, {}, {}
    for e in range(3):
        for f in range(3):
            for a in range(-1, 4):
                inside = 0 <= a < 3
                p1[a, e, f] = w1[a, e, f].astype(F32) if inside else zero1
                p2[a, e, f] = w2[a, e, f].astype(F32).T if inside else zero2
                p3[a, e, f] = w3[a, e, f].astype(F32) if inside else zero3
    join = lambda pieces: jnp.concatenate(pieces, axis=1).astype(BF)
    for xo in range(2):
        for f in range(3):
            for e in range(3):
                v = join([p1[xi - xo, e, f] for xi in range(4)])
                a1[pl.ds((xo * 3 + f) * n1, n1), pl.ds(e * 4 * n1, 4 * n1)] = v
                a1s[pl.ds(((xo * 3 + e) * 3 + f) * n1, n1), :] = v
            for h in range(2):
                for e in range(3):
                    spot = pl.ds((e * 3 + f) * 2 * n2, 2 * n2)
                    a3[h, pl.ds(xo * n2, n2), spot] = join([p3[2 * h + r - xo, e, f] for r in range(2)])
    for h in range(2):
        for xo in range(2):
            row = [p2[2 * h + r - xo, e, f] for e in range(3) for f in range(3) for r in range(2)]
            a2[h, pl.ds(xo * n2, n2), :] = join(row)
        for f in range(3):
            a1h[h, pl.ds(f * n1, n1), :] = join([p1[2 * h, e, f] for e in range(3)])
    for b, c in ((b1, c1), (b2, c2), (b3, c3)):
        n = b.shape[1]
        eye = lax.broadcasted_iota(jnp.int32, (n, n), 0) == lax.broadcasted_iota(jnp.int32, (n, n), 1)
        column = jnp.sum(jnp.where(eye, jnp.broadcast_to(b[...], (n, n)), 0.0), axis=1, keepdims=True)
        c[...] = jnp.broadcast_to(column, c.shape)
    src = lax.broadcasted_iota(jnp.int32, evens.shape, 0)
    dst = lax.broadcasted_iota(jnp.int32, evens.shape, 1)
    evens[...] = jnp.where(src == 2 * dst, 1.0, 0.0).astype(BF)
    half = evens.shape[1]
    top = half - 2 * G
    src = lax.broadcasted_iota(jnp.int32, ends.shape, 0) - top
    dst = lax.broadcasted_iota(jnp.int32, ends.shape, 1)
    move = (
        ((dst == 0) & (src == 5))
        | ((dst == half - 1) & (src == G + 1))
        | ((dst == half) & (src == G + 3))
        | ((dst == half + 1) & (src == G + 5))
        | ((dst == 254) & (src == 1))
        | ((dst == 255) & (src == 3))
    )
    ends[...] = jnp.where(move, 1.0, 0.0).astype(BF)


def relayout(cells, lo, hi, store):
    chans, depth, cross = cells.shape
    flat = cells.astype(F32).reshape(chans * depth, cross)
    lo[...] = flat[:, :128]
    hi[...] = flat[:, 128:]
    lane = lanes((chans, 128))
    left = jnp.zeros((chans, 128), F32)
    right = jnp.zeros((chans, 128), F32)
    for z in range(depth):
        a = lo[pl.ds(z, chans, stride=depth), :]
        b = hi[pl.ds(z, chans, stride=depth), :]
        store(z, a.astype(BF), b.astype(BF))
        here = (lane >= z * G) & (lane < z * G + G)
        left = jnp.where(here, roll(a, z * G), left)
        right = jnp.where(here, roll(b, z * G + G), right)
    part = lane % G
    msg_l = jnp.where(part >= 3, roll(left, 3), 0.0).astype(BF)
    own_l = jnp.where(part >= 5, roll(left, 5), 0.0).astype(BF)
    msg_r = jnp.where(part < 5, roll(right, -3), 0.0).astype(BF)
    own_r = jnp.where(part < 3, roll(right, -5), 0.0).astype(BF)
    return msg_l, msg_r, own_l, own_r


def row_kernel(image, local, far_row, far_small, lo, hi, sems):
    inline = image.shape[1]
    far = (inline - 1) * (lax.axis_index("gx") % 2)
    copies = []
    for k in range(inline):
        x = (far + k) % inline
        copies.append(pltpu.make_async_copy(image.at[:, x], local.at[x], sems.at[k]))
        copies[k].start()
    copies[0].wait()

    def store(z, a, b):
        far_row[z, :, :128] = a
        far_row[z, :, 128:] = b

    msg_l, msg_r, own_l, own_r = relayout(local[far], lo, hi, store)
    far_small[0, :, :128] = msg_l
    far_small[0, :, 128:] = msg_r
    far_small[1, :, :128] = own_l
    far_small[1, :, 128:] = own_r
    for copy in copies[1:]:
        copy.wait()


def near_kernel(local, near_row, lo, hi):
    inline, _, depth, _ = local.shape
    near = (inline - 1) * (1 - lax.axis_index("gx") % 2)

    def store(z, a, b):
        near_row[z, :, :128] = a
        near_row[z, :, 128:] = b

    msg_l, msg_r, own_l, own_r = relayout(local[near], lo, hi, store)
    near_row[depth, :, :128] = msg_l
    near_row[depth, :, 128:] = msg_r
    near_row[depth + 1, :, :128] = own_l
    near_row[depth + 1, :, 128:] = own_r


def pack_kernel(local, near_row, far_row, far_small, own, msgs, olds, lo, hi):
    inline, _, depth, _ = local.shape
    odd = lax.axis_index("gx") % 2
    near, far = (inline - 1) * (1 - odd), (inline - 1) * odd
    own[:, far] = far_row[...]
    msgs[far] = far_small[0]
    olds[far] = far_small[1]
    own[:, near] = near_row[pl.ds(0, depth)]
    msgs[near] = near_row[depth]
    olds[near] = near_row[depth + 1]
    for x in range(1, inline - 1):

        def store(z, a, b):
            own[z, x, :, :128] = a
            own[z, x, :, 128:] = b

        msg_l, msg_r, own_l, own_r = relayout(local[x], lo.at[x - 1], hi.at[x - 1], store)
        msgs[x, :, :128] = msg_l
        msgs[x, :, 128:] = msg_r
        olds[x, :, :128] = own_l
        olds[x, :, 128:] = own_r


def at_map_end():
    at = lax.axis_index("gx")
    return (at == 0) | (at == lax.axis_size("gx") - 1)


def strip_kernel(far_row, mate, msgs, olds, send_1, send_2, strips):
    inline = msgs.shape[0]
    depth = mate.shape[0] - 2
    odd = lax.axis_index("gx") % 2
    outside = at_map_end()
    far, near = (inline + 1) * odd, (inline + 1) * (1 - odd)
    zero = jnp.zeros(strips.shape[1:], BF)
    far_msg = jnp.where(outside, zero, far_row[0])
    near_msg = mate[depth]
    strips[pl.ds(1, inline)] = olds[...]
    strips[near] = mate[depth + 1]
    strips[far] = jnp.where(outside, zero, far_row[1])
    for send, right in ((send_1, odd == 0), (send_2, odd == 1)):

        def pick(v):
            return jnp.where(right, v[..., 128:], v[..., :128])

        send[pl.ds(1, inline)] = pick(msgs[...])
        send[near] = pick(near_msg)
        send[far] = pick(far_msg)


def taps(g, rows):
    return roll(g[:rows], 1) + g[rows : 2 * rows] + roll(g[2 * rows :], -1)


def finish(z, m, bias, acc):
    m = jnp.maximum(jnp.maximum(m, roll(m, -1)) + bias[...], 0.0)
    rows = m.shape[0]
    acc[pl.ds(z * rows, rows), :] = m.astype(BF)


def fill(own, halo, halo_first, pad):
    depth, inline, chans, cross = own.shape
    width = inline * chans
    zero = jnp.zeros((width, cross), BF)
    pad[pl.ds(0, width), :] = zero
    pad[pl.ds((depth + 1) * width, width), :] = zero
    first = 1 - halo_first
    for z in range(depth):
        base = (z + 1) * width
        beyond = zero[:chans] if halo is None else halo[z]
        pad[pl.ds(pl.multiple_of(base + (1 - halo_first) * (inline - 1) * chans, chans), chans), :] = beyond
        for r in range(inline - 1):
            pad[pl.ds(pl.multiple_of(base + (r + halo_first) * chans, chans), chans), :] = own[z, first + r]


def layer_rows(z, a1, pad, width):
    g = dot(a1[...], pad[pl.ds(z * width, 3 * width), :])
    rows = g.shape[0] // 6
    return [taps(g[xo * 3 * rows : (xo + 1) * 3 * rows], rows) for xo in range(2)]


def early_kernel(own, mate, a1, bias, evens, pooled, sums, pad, rest, acc):
    depth, inline, chans, _ = own.shape
    width = inline * chans
    odd = lax.axis_index("gx") % 2
    fill(own, mate, odd, pad)
    fill(own, None, 1 - odd, rest)

    def layer(z):
        rows = layer_rows(z, a1, pad, width)
        return jnp.maximum(rows[0], rows[1])

    for z in range(depth // 2):
        finish(z, jnp.maximum(layer(2 * z), layer(2 * z + 1)), bias, acc)
    pooled[...] = dot(acc[...], evens[...]).astype(BF).reshape(pooled.shape)
    for z in range(depth):
        rows = layer_rows(z, a1, rest, width)
        sums[z, 0] = rows[0]
        sums[z, 1] = rows[1]


def late_kernel(
    sums, halo, early, strips, got_1, got_2, a1h, a1s, bias, evens, message, far_message, pad, acc, edges, rows
):
    depth, _, chans, cross = sums.shape
    half_depth = depth // 2
    odd = lax.axis_index("gx") % 2
    outside = at_map_end()
    edge_columns(strips, got_1, got_2, a1s, bias, edges, rows)
    zero = jnp.zeros((chans, cross), BF)
    pad[pl.ds(0, chans), :] = zero
    pad[pl.ds((depth + 1) * chans, chans), :] = zero
    for z in range(depth):
        pad[pl.ds((z + 1) * chans, chans), :] = jnp.where(outside, zero, halo[z])

    def layer(z):
        g = dot(a1h[odd], pad[pl.ds(z * chans, 3 * chans), :])
        return jnp.maximum(sums[z, odd] + taps(g, chans), sums[z, 1 - odd])

    for z in range(half_depth):
        finish(z, jnp.maximum(layer(2 * z), layer(2 * z + 1)), bias, acc)
    late = dot(acc[...], evens[...]).astype(BF).reshape(early.shape)
    message[odd, pl.ds(0, half_depth)] = late
    message[1 - odd, pl.ds(0, half_depth)] = early[...]
    message[0, half_depth] = edges[0]
    message[1, half_depth] = edges[1]
    far_message[pl.ds(0, half_depth)] = late
    far_message[half_depth] = edges[0]
    far_message[half_depth + 1] = edges[1]


def edge_columns(strips, got_1, got_2, a1s, bias, edges, rows):
    tall, chans, _ = strips.shape
    odd = lax.axis_index("gx") % 2
    at, end = lax.axis_index("gy"), lax.axis_size("gy") - 1
    part = lanes((tall * chans, 128)) % G
    one, two = got_1[...].reshape(tall * chans, 128), got_2[...].reshape(tall * chans, 128)
    from_l = jnp.where(at == 0, 0.0, jnp.where(odd == 0, one, two))
    from_r = jnp.where(at == end, 0.0, jnp.where(odd == 0, two, one))
    s = strips[...].reshape(tall * chans, 256)
    rows[:, :128] = jnp.where(part < 5, from_l, s[:, :128]).astype(BF)
    rows[:, 128:] = jnp.where(part < 3, s[:, 128:], from_r).astype(BF)
    lane = lanes((chans, 128))
    for pair in range(2):
        g = dot(a1s[...], rows[pl.ds(pair * 2 * chans, 4 * chans), :])
        sides = []
        for side in range(2):
            best = None
            for xo in range(2):
                total = None
                for e in range(3):
                    part = None
                    for f in range(3):
                        k = (xo * 3 + e) * 3 + f
                        t = g[k * chans : (k + 1) * chans, side * 128 : side * 128 + 128]
                        t = roll(t, -(G * (e - 1) + f - 1))
                        part = t if part is None else part + t
                    if e == 0:
                        part = jnp.where(lane >= G, part, 0.0)
                    if e == 2:
                        part = jnp.where(lane < 128 - G, part, 0.0)
                    total = part if total is None else total + part
                best = total if best is None else jnp.maximum(best, total)
            best = jnp.maximum(best, roll(best, -G))
            best = jnp.maximum(best, roll(best, -1))
            best = jnp.maximum(best + bias[:, :128], 0.0)
            cell = lane % G
            outside = (cell < 5) & (at == 0) if side == 0 else (cell > 1) & (at == end)
            sides.append(jnp.where(outside, 0.0, best))
        edges[pair] = jnp.where((lane // G) % 2 == 0, sides[0], roll(sides[1], G)).astype(BF)


def assemble(cells, columns, depth, ends, outside, q2, eb):
    coarse = 2
    half = eb.shape[1]
    chans = q2.shape[0] // (depth + 1) // 6
    width = coarse * chans
    zero = jnp.zeros((chans, half), BF)

    def hide(v):
        return v if outside is None else jnp.where(outside, zero, v)

    edge = jnp.concatenate([hide(columns(r)) for r in range(coarse)], axis=0)
    flat = edge.astype(F32)
    lane = lanes((width, half))
    for e in range(3):
        for f in range(3):
            by = 2 * G * (e - 1) + 2 * (f - 1)
            v = roll(flat, -by) if by else flat
            if e == 0:
                v = jnp.where(lane >= 2 * G, v, 0.0)
            if e == 2:
                v = jnp.where(lane < half - 2 * G, v, 0.0)
            eb[pl.ds((e * 3 + f) * width, width), :] = v.astype(BF)
    clear(q2, depth)
    lane = lanes((chans, half))
    inner = (lane > 0) & (lane < half - 1)
    for z in range(depth):
        fixed = dot(edge, ends[pl.ds(half - 2 * G - 2 * G * z, half), :])
        for r in range(coarse):
            own = fixed[r * chans : (r + 1) * chans]
            main = jnp.where(inner, hide(cells(r, z)).astype(F32), own[:, :half])
            keep(q2, z, r, jnp.concatenate([main, own[:, half:]], axis=1))


def keep(q, z, r, v):
    rows = v.shape[0]
    half = v.shape[1] // 2
    for f in range(3):
        s = v if f == 1 else roll(v, 1 - f)
        s = s[:, :half].astype(BF)
        q[pl.ds(((z * 3 + f) * 2 + r) * rows, rows), half:] = s
        q[pl.ds((((z + 1) * 3 + f) * 2 + r) * rows, rows), :half] = s


def clear(q, depth):
    rows = q.shape[0] // (depth + 1)
    half = q.shape[1] // 2
    q[pl.ds(0, rows), :half] = jnp.zeros((rows, half), BF)
    q[pl.ds(depth * rows, rows), half:] = jnp.zeros((rows, half), BF)


def coarse_own_kernel(own, a2, ends, near, near_ends, part2, part2_ends, q2, eb):
    _, tall, chans, _ = own.shape
    depth = tall - 1
    odd = lax.axis_index("gx") % 2
    assemble(lambda r, z: own[r, z], lambda r: own[r, depth], depth, ends, None, q2, eb)
    rows = 6 * chans
    for part, into, into_ends in ((odd, near, near_ends), (1 - odd, part2, part2_ends)):
        for z in range(0, depth, 2):
            into[z // 2] = dot(a2[part], q2[pl.ds(z * rows, 3 * rows), :])
        into_ends[...] = dot(a2[part], eb[...])


def first_map(part, a2, b2, add, add_ends, outside, q2, eb, q, depth):
    half = eb.shape[1]
    c2 = b2.shape[0]
    at, end = lax.axis_index("gy"), lax.axis_size("gy") - 1
    rows = q2.shape[0] // (depth + 1)
    lane = lanes((c2, half))
    left = (lane % (2 * G)) < G
    beyond = (left & (at == 0)) | (~left & (at == end))
    clear(q, depth)
    g = dot(a2[part], eb[...]) + add_ends[...]
    ends = []
    for xo in range(2):
        v = jnp.maximum(g[xo * c2 : (xo + 1) * c2] + b2[:, :half], 0.0)
        ends.append(jnp.where(beyond, 0.0, v))
    for z in range(0, depth, 2):
        g = dot(a2[part], q2[pl.ds(z * rows, 3 * rows), :]) + add[z // 2]
        for xo in range(2):
            v = jnp.maximum(g[xo * c2 : (xo + 1) * c2] + b2[...], 0.0)
            for k in range(2):
                spot = 2 * G * (z + k) + 3
                right = roll(ends[xo], -(spot + G))
                before = roll(ends[xo], half - 1 - spot)
                side = jnp.where(lane == 0, right, before)
                w = jnp.concatenate([v[:, k * half : (k + 1) * half], side], axis=1)
                if outside is not None:
                    w = jnp.where(outside[xo], 0.0, w)
                keep(q, z + k, xo, w)


def coarse_near_kernel(mate, near, near_ends, a2, b2, a3, ends, part3, q2, eb, q):
    _, tall, _, _ = mate.shape
    depth = tall - 1
    c2 = b2.shape[0]
    odd = lax.axis_index("gx") % 2
    assemble(lambda r, z: mate[r, z], lambda r: mate[r, depth], depth, ends, None, q2, eb)
    first_map(1 - odd, a2, b2, near, near_ends, None, q2, eb, q, depth)
    rows = 6 * c2
    for z in range(0, depth, 2):
        part3[z // 2] = dot(a3[1 - odd], q[pl.ds(z * rows, 3 * rows), :])


def coarse_far_kernel(first, far, part2, part2_ends, part3, a2, b2, a3, b3, ends, out, q2, eb, q, wide):
    depth, _, half = first.shape
    coarse = out.shape[1]
    c2 = b2.shape[0]
    odd = lax.axis_index("gx") % 2
    at, end = lax.axis_index("gx"), lax.axis_size("gx") - 1

    def cells(r, z):
        return jnp.where(odd == r, first[z], far[z])

    assemble(cells, lambda r: far[depth + r], depth, ends, at_map_end(), q2, eb)
    outside = [(odd == 0) & (at == 0), (odd == 1) & (at == end)]
    first_map(odd, a2, b2, part2, part2_ends, outside, q2, eb, q, depth)
    rows = 6 * c2
    for z in range(0, depth, 2):
        g = dot(a3[odd], q[pl.ds(z * rows, 3 * rows), :]) + part3[z // 2]
        for xo in range(2):
            v = jnp.maximum(g[xo * c2 : (xo + 1) * c2] + b3[...], 0.0)
            wide[xo, pl.ds(z, c2, stride=depth), :] = v[:, :half]
            wide[xo, pl.ds(z + 1, c2, stride=depth), :] = v[:, half:]
    for xo in range(coarse):
        out[:, xo] = wide[xo].reshape(c2, depth, half).astype(BF)


def permute(value, target):
    wide, deep = lax.axis_size("gx"), lax.axis_size("gy")
    pairs = []
    for x in range(wide):
        for y in range(deep):
            tx, ty = target(x, y, wide, deep)
            pairs.append((x * deep + y, tx * deep + ty))
    return lax.ppermute(value, ("gx", "gy"), pairs)


def mate_of(x, y, wide, deep):
    return x ^ 1, y


def far_of(x, y, wide, deep):
    to = x + 1 if x % 2 else x - 1
    if 0 <= to < wide:
        return to, y
    if deep % 2 == 0:
        return x, y ^ 1
    return to % wide, y


def loop_of(up):
    def target(x, y, wide, deep):
        to = y + 1 if (x % 2 == 0) == up else y - 1
        return (x, to) if 0 <= to < deep else (x ^ 1, y)

    return target


def per_device(image, w_first, b_first, w_second, b_second, w_third, b_third):
    c1, inline, depth, cross = image.shape
    c2 = w_third.shape[0]
    half, hz, coarse = cross // 2, depth // 2, inline // 2
    k1 = 4 * c1
    tall = inline + 2
    local, far_row, far_small = call(
        row_kernel,
        [((inline, c1, depth, cross), BF), ((depth, c1, cross), BF), ((2, c1, 256), BF)],
        scratch=[pltpu.VMEM((c1 * depth, 128), F32)] * 2 + [pltpu.SemaphoreType.DMA((inline,))],
        flops=1 << 20,
        space=pltpu.MemorySpace.HBM,
        limit=52,
    )(image)
    got_small = permute(far_small, far_of)
    got_far = permute(far_row, far_of)
    (near_row,) = call(
        near_kernel, [((depth + 2, c1, cross), BF)], scratch=[pltpu.VMEM((c1 * depth, 128), F32)] * 2, flops=1 << 27
    )(local)
    own, msgs, olds = call(
        pack_kernel,
        [((depth, inline, c1, cross), BF), ((inline, c1, 256), BF), ((inline, c1, 256), BF)],
        scratch=[pltpu.VMEM((inline - 2, c1 * depth, 128), F32)] * 2,
        flops=1 << 28,
    )(local, near_row, far_row, far_small)
    got_row = permute(near_row, mate_of)
    a1, a1s, a1h, a2, a3, b1, b2, b3, evens, ends = call(
        weights_kernel,
        [
            ((6 * c1, 3 * k1), BF),
            ((18 * c1, k1), BF),
            ((2, 3 * c1, 3 * c1), BF),
            ((2, 2 * c2, 18 * c1), BF),
            ((2, 2 * c2, 18 * c2), BF),
            ((c1, 256), F32),
            ((c2, 256), F32),
            ((c2, 256), F32),
            ((cross, half), BF),
            ((2 * half, 256), BF),
        ],
        flops=1 << 28,
    )(
        jnp.transpose(w_first, (2, 3, 4, 0, 1)),
        jnp.transpose(w_second, (2, 3, 4, 1, 0)),
        jnp.transpose(w_third, (2, 3, 4, 0, 1)),
        b_first.reshape(1, c1),
        b_second.reshape(1, c2),
        b_third.reshape(1, c2),
    )
    fine = [pltpu.VMEM(((depth + 2) * k1, cross), BF), pltpu.VMEM((hz * c1, cross), BF)]
    early, sums = call(
        early_kernel, [((hz, c1, half), BF), ((depth, 2, c1, cross), F32)], scratch=fine[:1] + fine, flops=1 << 30
    )(own, got_row, a1, b1, evens)
    send_1, send_2, strips = call(
        strip_kernel, [((tall, c1, 128), BF)] * 2 + [((tall, c1, 256), BF)], flops=1 << 20
    )(got_small, got_row, msgs, olds)
    got_1 = permute(send_1, loop_of(True))
    got_2 = permute(send_2, loop_of(False))
    got_first = permute(early, far_of)
    message, far_message = call(
        late_kernel,
        [((coarse, hz + 1, c1, half), BF), ((hz + 2, c1, half), BF)],
        scratch=[
            pltpu.VMEM(((depth + 2) * c1, cross), BF),
            pltpu.VMEM((hz * c1, cross), BF),
            pltpu.VMEM((coarse, c1, half), BF),
            pltpu.VMEM((tall * c1, 256), BF),
        ],
        flops=1 << 28,
    )(sums, got_far, early, strips, got_1, got_2, a1h, a1s, b1, evens)
    got_pa = permute(message, mate_of)
    got_pb = permute(far_message, far_of)
    q2 = pltpu.VMEM(((hz + 1) * 6 * c1, 256), BF)
    eb = pltpu.VMEM((18 * c1, half), BF)
    q = pltpu.VMEM(((hz + 1) * 6 * c2, 256), BF)
    sums2 = [((hz // 2, 2 * c2, 256), F32), ((2 * c2, half), F32)]
    near, near_ends, part2, part2_ends = call(
        coarse_own_kernel, sums2 * 2, scratch=[q2, eb], flops=1 << 29
    )(message, a2, ends)
    (part3,) = call(
        coarse_near_kernel, [((hz // 2, 2 * c2, 256), F32)], scratch=[q2, eb, q], flops=1 << 29
    )(got_pa, near, near_ends, a2, b2, a3, ends)
    (out,) = call(
        coarse_far_kernel,
        [((c2, coarse, hz, half), BF)],
        scratch=[q2, eb, q, pltpu.VMEM((coarse, c2 * hz, half), F32)],
        flops=1 << 29,
    )(got_first, got_pb, part2, part2_ends, part3, a2, b2, a3, b3, ends)
    return out


def solution(mesh):
    placed = (P(None, "gx", None, "gy"), P(), P(), P(), P(), P(), P())

    return jax.shard_map(per_device, mesh=mesh, in_specs=placed, out_specs=P(None, "gx", None, "gy"), check_vma=False)
```
